32 devices in a mesh: freq: 4 (over y, x), band: 8 (over z, core).
Axes of the slice: x: 2, y: 2, z: 4, core: 2. Of those that a mesh axis runs over, the one named last changes fastest.
Arguments:
- pair_density: bfloat16 [1024, 2, 8192], P(('freq', 'band')), may hold values from -6 to 6
- trial_vectors: bfloat16 [16, 2, 64, 8192], P('freq', None, None, 'band'), may hold values from -6 to 6
- frequency: float32 [16], P('freq'), may hold values from 0.05 to 20
- val_energy: float32 [32], replicated, may hold values from -3 to -0.1
- cond_energy: float32 [32], replicated, may hold values from 0.1 to 4
- pair_index: int32 [1024], P(('freq', 'band')), may hold values from 0 to 1023, each once
Outputs:
- images: float32 [16, 2, 64, 8192], P('freq', None, None, 'band')
- subspace: float32 [16, 2, 64, 64], P('freq')
The draws below stay inside these ranges and needn't reach their ends.
Inputs may be any that keep to these rules, and one draw needn't show every extreme that they name: `pair_index`: every pair number 0 to 1023 appears exactly once.
All inputs are finite; a program needn't handle non-finite values.
Results may differ from the reference program's by a relative error of at most 0.0085.
Values may be sent and summed in bfloat16 or wider, within the bound.
A program may use at most 128 MiB of HBM per device.

```python
import math
import jax
import jax.numpy as jnp
from jax import lax

NG = 8192
NV = 32
K = 64
NFREQ = 16
PAIRS = 1024
NC = 32


def block_scale(own_key, dims, shards, smallest, top_value):
    gain = 1.0
    for position, shards_of in shards:
        draws = jax.random.uniform(jax.random.fold_in(jax.random.fold_in(own_key, 6), position), (shards_of,), jnp.float32, smallest / len(shards), top_value / len(shards))
        gain = gain * jnp.repeat(jnp.exp(draws), dims[position] // shards_of).reshape((-1,) + (1,) * (len(dims) - 1 - position))
    return gain


def bell_draw(rng, extent, spread, most, shards=(), kind=jnp.bfloat16):
    loudness = block_scale(rng, extent, shards, -0.22, 0.18) if shards else 1.0
    array = jax.random.normal(rng, extent, jnp.float32) * spread * loudness
    return jnp.minimum(jnp.maximum(array, -most), most).astype(kind)


def setup_inputs(seed: int = 0) -> dict:
    keys = jax.random.split(jax.random.key(seed), 7)
    pair_density = bell_draw(keys[0], (PAIRS, 2, NG), 1.0, 6.0, ((0, 32),))
    trial_vectors = bell_draw(keys[1], (NFREQ, 2, K, NG), 1.0, 6.0, ((0, 4), (3, 8)))
    frequency = jnp.clip(jnp.exp(math.log(20.0) - 5.9914645 * jax.random.uniform(keys[2], (NFREQ,), jnp.float32) ** block_scale(keys[2], (NFREQ,), ((0, 4),), -0.2, 0.2)), 0.05, 20.0)
    val_energy = jnp.clip(jax.random.uniform(keys[3], (NV,), jnp.float32, -3.0, -0.1), -3.0, -0.1)
    cond_energy = jnp.clip(jax.random.uniform(keys[4], (NC,), jnp.float32, 0.1, 4.0), 0.1, 4.0)
    pair_index = jax.random.permutation(keys[5], PAIRS).astype(jnp.int32)
    return dict(pair_density=pair_density, trial_vectors=trial_vectors, frequency=frequency, val_energy=val_energy, cond_energy=cond_energy, pair_index=pair_index)


def pair_weights(pair_index, frequency, val_energy, cond_energy):
    delta = cond_energy[pair_index % NC] - val_energy[pair_index // NC]
    prefactor = 1.0 / math.sqrt(2.0 * NG * PAIRS)
    ratio = delta[None, :] / (delta[None, :] * delta[None, :] + frequency[:, None] * frequency[:, None])
    return (-4.0 * prefactor * ratio).astype(jnp.bfloat16)

def reference(pair_density, trial_vectors, frequency, val_energy, cond_energy, pair_index):
    density = pair_density.astype(jnp.float32)
    vectors = trial_vectors.astype(jnp.float32)
    weight = pair_weights(pair_index, frequency, val_energy, cond_energy).astype(jnp.float32)
    products = jnp.einsum('pcg,fekg->fcekp', density, vectors)
    over_real = products[:, 0, 0] + products[:, 1, 1]
    over_imag = products[:, 0, 1] - products[:, 1, 0]
    scaled_real = (weight[:, None, :] * over_real).astype(jnp.bfloat16)
    scaled_imag = (weight[:, None, :] * over_imag).astype(jnp.bfloat16)
    mixed = jnp.stack([jnp.stack([scaled_real, -scaled_imag], 1), jnp.stack([scaled_imag, scaled_real], 1)], 1)
    images = jnp.einsum('pcg,fdckp->fdkg', density, mixed.astype(jnp.float32))
    hp = lax.Precision.HIGHEST
    real_part = jnp.einsum('fkg,flg->fkl', vectors[:, 0], images[:, 0], precision=hp) + jnp.einsum('fkg,flg->fkl', vectors[:, 1], images[:, 1], precision=hp)
    imag_part = jnp.einsum('fkg,flg->fkl', vectors[:, 0], images[:, 1], precision=hp) - jnp.einsum('fkg,flg->fkl', vectors[:, 1], images[:, 0], precision=hp)
    subspace = jnp.stack([real_part, imag_part], 1) / NG
    return (images, subspace)
```

```python
import functools
import math

import jax
import jax.numpy as jnp
from jax import lax
from jax.experimental import pallas as pl
from jax.experimental.pallas import tpu as pltpu
from jax.sharding import PartitionSpec as P

MESH = pl.DeviceIdType.MESH
F32 = jnp.float32
BF16 = jnp.bfloat16


def kernel(
    groups, members, chunks, freqs, vecs, rows, grid_here, prefactor, inv_grid,
    dens, trial, frequency, val_energy, cond_energy, pair_index,
    images, sub,
    raw, packed, total_own, held, both, delta_own, freq_row, deltas, cols, ring_out, ring_in, scaled, acc,
    other, late_out, late_in, sub_out, sub_in,
    sem_in, sem_out, sem_as, sem_ar, sem_os, sem_or, sem_fs, sem_fr, sem_ds, sem_dr, sem_es, sem_er,
    sem_rs, sem_rr, sem_gs, sem_gr, sem_is, sem_ir,
):
    f = lax.axis_index("freq")
    b = lax.axis_index("band")
    chips = members // 2
    piece = rows // chunks
    zc = b // 2
    core = b % 2
    width = freqs * 2 * vecs
    slot = groups * piece
    chunk_rows = chips * slot
    wide = 2 * grid_here
    partner = zc * 2 + (1 - core)

    def remote(src, dst, send, recv, freq_id, band_id):
        return pltpu.make_async_remote_copy(
            src_ref=src, dst_ref=dst, send_sem=send, recv_sem=recv,
            device_id=(freq_id, band_id), device_id_type=MESH,
        )

    def peer(s):
        return (zc + s) % chips * 2 + core

    barrier = pltpu.get_barrier_semaphore()
    pl.semaphore_signal(barrier, inc=1, device_id=(f, partner), device_id_type=MESH)
    for s in range(1, chips):
        pl.semaphore_signal(barrier, inc=1, device_id=(f, peer(s)), device_id_type=MESH)
    for s in range(1, groups):
        pl.semaphore_signal(barrier, inc=1, device_id=((f + s) % groups, b), device_id_type=MESH)

    def load(c):
        return pltpu.make_async_copy(
            dens.at[pl.ds(c * piece, piece)], raw.at[pl.ds(c * piece, piece)], sem_in.at[c]
        )

    for c in range(chunks):
        load(c).start()
    pltpu.make_async_copy(trial, both.at[:, pl.ds(pl.multiple_of(core * grid_here, 128), grid_here)], sem_os.at[1]).start()

    def pack(c):
        load(c).wait()
        packed[c] = jnp.swapaxes(raw[c * piece : (c + 1) * piece], 0, 1).reshape(2 * piece, -1)

    def ready():
        pl.semaphore_wait(barrier, chips + groups - 1)

    def waves(c, z):
        return packed.at[c, :, pl.ds(pl.multiple_of(z * wide, 128), wide)]

    sends = []

    def go(copy):
        copy.start()
        sends.append(copy)

    def exchange(c):
        for r in range(1, chips):
            z = (zc + r) % chips
            go(remote(waves(c, z), held.at[c, f, zc], sem_as.at[c, r], sem_ar.at[c, zc], f, peer(r)))

    square_groups = groups == 4
    xx, yy = f % 2, f // 2
    fx, fy = yy * 2 + (1 - xx), (1 - yy) * 2 + xx
    fd = (1 - yy) * 2 + (1 - xx)

    def piece_copy(c, g, z, lane, to):
        ref = held.at[c, g, z]
        return remote(ref, ref, sem_fs.at[c, lane, z], sem_fr.at[c, lane, z], to, b)

    def whole(c, g, lane, to):
        return remote(held.at[c, g], held.at[c, g], sem_fs.at[c, lane, 0], sem_fr.at[c, lane, 0], to, b)

    def own_send(c):
        keep = pltpu.make_async_copy(waves(c, zc), held.at[c, f, zc], sem_ar.at[c, zc])
        keep.start()
        if square_groups:
            for lane, to in ((0, fx), (1, fy)):
                go(remote(waves(c, zc), held.at[c, f, zc], sem_fs.at[c, lane, zc], sem_fr.at[c, lane, zc], to, b))

    def landed(c, z):
        pltpu.make_async_copy(waves(c, 0), held.at[c, f, z], sem_ar.at[c, z]).wait()

    def spread(c, offsets):
        for r in offsets:
            z = (zc + r) % chips
            landed(c, z)
            if square_groups:
                go(piece_copy(c, f, z, 0, fx))
                go(piece_copy(c, f, z, 1, fy))
        if not square_groups and offsets and offsets[-1] == chips - 1:
            landed(c, zc)
            for s in range(1, groups):
                go(whole(c, f, s, (f + s) % groups))

    def relay(c, offsets):
        if square_groups:
            for r in offsets:
                z = (zc + r) % chips
                if (r + c) % 2 == 0:
                    piece_copy(c, fx, z, 0, fx).wait_recv()
                    go(piece_copy(c, fx, z, 2, fy))
                else:
                    piece_copy(c, fy, z, 1, fy).wait_recv()
                    go(piece_copy(c, fy, z, 3, fx))

    def arrive(c):
        if square_groups:
            landed(c, zc)
            for r in range(chips):
                z = (zc + r) % chips
                if (r + c) % 2 == 0:
                    piece_copy(c, fy, z, 1, fy).wait_recv()
                    piece_copy(c, fd, z, 2, fy).wait_recv()
                else:
                    piece_copy(c, fx, z, 0, fx).wait_recv()
                    piece_copy(c, fd, z, 3, fx).wait_recv()
        else:
            for s in range(1, groups):
                src = (f + groups - s) % groups
                whole(c, src, s, src).wait_recv()

    def half_of(ref, k):
        return ref.at[:, pl.ds(pl.multiple_of(k * grid_here, 128), grid_here)]

    def vectors_send():
        go(remote(trial, half_of(both, core), sem_os.at[0], sem_or.at[0], f, partner))

    def vectors():
        pltpu.make_async_copy(trial, half_of(both, core), sem_os.at[1]).wait()
        remote(trial, half_of(both, 1 - core), sem_os.at[0], sem_or.at[0], f, partner).wait_recv()

    def energies():
        cond_count = cond_energy.shape[0]
        val_count = val_energy.shape[0]
        index = pair_index[...]
        rest_index = index
        val_pick = jnp.full(index.shape, val_energy[0], F32)
        for v in range(1, val_count):
            above = index >= v * cond_count
            val_pick = jnp.where(above, val_energy[v], val_pick)
            rest_index = jnp.where(above, index - v * cond_count, rest_index)
        cond_pick = jnp.full(index.shape, cond_energy[0], F32)
        for v in range(1, cond_count):
            cond_pick = jnp.where(rest_index == v, cond_energy[v], cond_pick)
        delta_own[...] = jnp.ones_like(delta_own)
        delta_own[0:1, 0:rows] = cond_pick - val_pick
        for q in range(freqs):
            freq_row[:, q * 2 * vecs : (q + 1) * 2 * vecs] = jnp.full((1, 2 * vecs), frequency[q], F32)
        pltpu.make_async_copy(delta_own, deltas.at[f, zc], sem_dr.at[zc]).start()
        for s in range(1, chips):
            go(remote(delta_own, deltas.at[f, zc], sem_ds.at[s], sem_dr.at[zc], f, peer(s)))

    def pass_deltas():
        for j in range(chips):
            pltpu.make_async_copy(delta_own, deltas.at[f, j], sem_dr.at[j]).wait()
        for s in range(1, groups):
            go(remote(deltas.at[f], deltas.at[f], sem_es.at[s], sem_er.at[s], (f + s) % groups, b))

    def columns():
        for s in range(1, groups):
            src = (f + groups - s) % groups
            remote(deltas.at[src], deltas.at[src], sem_es.at[s], sem_er.at[s], src, b).wait_recv()
        for g in range(groups):
            for j in range(chips):
                turned = jnp.transpose(deltas[g, j])
                at = (g * chips + j) * piece
                for c in range(chunks):
                    cols[c, at : at + piece, :] = turned[c * piece : (c + 1) * piece, :]

    hw = width // 2

    def weights(column, h):
        freq = freq_row[:, h * hw : (h + 1) * hw]
        ratio = column / (column * column + freq * freq)
        return (-4.0 * prefactor * ratio).astype(BF16).astype(F32)

    lane_at = lax.broadcasted_iota(jnp.int32, (1, 2 * vecs), 1)

    def swap(x, low, high):
        sign = jnp.where(lane_at < vecs, low, high)
        return jnp.concatenate(
            [
                pltpu.roll(x[:, q * 2 * vecs : (q + 1) * 2 * vecs], vecs, 1) * sign
                for q in range(freqs // 2)
            ],
            axis=1,
        )

    def cross(j, h):
        if h == 0:
            arrive(j)
        over_grid = (((1,), (1,)), ((), ()))
        out = lax.dot_general(
            held[j].reshape(2 * chunk_rows, wide),
            both[h * hw : (h + 1) * hw, :],
            over_grid,
            preferred_element_type=F32,
        ).reshape(groups * chips, 2, piece, hw)
        total = out[:, 0].reshape(chunk_rows, hw) + swap(
            out[:, 1].reshape(chunk_rows, hw), 1.0, -1.0
        )
        ring_out[j, h] = total.astype(BF16).reshape(chips, slot, hw)
        if split(j) or h == 1:
            for s in range(1, chips):
                go(slot_copy(j, h, s, (zc + s) % chips))

    def split(j):
        return j == chunks - 1

    def slot_copy(j, h, s, at):
        if split(j):
            src, dst = ring_out.at[j, h, at], ring_in.at[j, h, s]
        else:
            src, dst, h = ring_out.at[j, :, at], ring_in.at[j, :, s], 0
        return remote(src, dst, sem_rs.at[j, h, s], sem_rr.at[j, h, s], f, peer(s))

    def scaled_copy(j, h, s, at):
        if split(j):
            ref = scaled.at[j, h, at]
        else:
            ref, h = scaled.at[j, :, at], 0
        return remote(ref, ref, sem_gs.at[j, h, s], sem_gr.at[j, h, s], f, peer(s))

    def scale(j, h):
        total = ring_out[j, h, zc].astype(F32)
        for s in range(1, chips):
            if split(j) or h == 0:
                slot_copy(j, h, s, zc).wait_recv()
            total = total + ring_in[j, h, s].astype(F32)
        column = cols[j, pl.ds(pl.multiple_of(zc * slot, 8), slot), 0:1]
        scaled[j, h, zc] = (weights(column, h) * total).astype(BF16)
        if split(j) or h == 1:
            for s in range(1, chips):
                go(scaled_copy(j, h, s, zc))

    def share(j, h):
        if split(j) or h == 0:
            for s in range(1, chips):
                scaled_copy(j, h, s, (zc + chips - s) % chips).wait_recv()

    over_rows = (((0,), (0,)), ((), ()))

    def paired(j, h):
        flat32 = scaled[j, h].reshape(chunk_rows, hw).astype(F32)
        turned = swap(flat32, -1.0, 1.0)
        return jnp.concatenate(
            [
                flat32.reshape(groups * chips, 1, piece, hw),
                turned.reshape(groups * chips, 1, piece, hw),
            ],
            axis=1,
        ).reshape(2 * chunk_rows, hw).astype(BF16)

    def term(j, left, k):
        right = held[j, :, :, :, pl.ds(pl.multiple_of(k * grid_here, 128), grid_here)]
        return lax.dot_general(
            left, right.reshape(2 * chunk_rows, grid_here), over_rows, preferred_element_type=F32
        )

    def squares(j, h):
        flat = scaled[j, h].reshape(chunk_rows, hw)
        column = cols[j, :, 0:1]
        crossing = (flat.astype(F32) / weights(column, h)).astype(BF16)
        for i in range(freqs // 2):
            lo, hi = i * 2 * vecs, (i + 1) * 2 * vecs
            q = h * (freqs // 2) + i
            square = lax.dot_general(
                crossing[:, lo:hi], flat[:, lo:hi], over_rows, preferred_element_type=F32
            )
            if j == 0:
                acc[q] = square
            else:
                acc[q] = acc[q] + square

    def image(j, h):
        left = paired(j, h)
        part = slice(h * hw, (h + 1) * hw)
        if j == 0:
            other[part, :] = term(j, left, 1 - core)
            total_own[part, :] = term(j, left, core)
        else:
            other[part, :] = other[part, :] + term(j, left, 1 - core)
            total_own[part, :] = total_own[part, :] + term(j, left, core)
        squares(j, h)

    quarter = width // 4

    def late_copy(k):
        part = pl.ds(k * quarter, quarter)
        return remote(late_out.at[part], late_in.at[part], sem_is.at[k], sem_ir.at[k], f, partner)

    def sub_copy():
        return remote(sub_out, sub_in, sem_is.at[4], sem_ir.at[4], f, partner)

    def last_other(h):
        j = chunks - 1
        left = paired(j, h)
        for i in range(2):
            k = 2 * h + i
            part = slice(k * quarter, (k + 1) * quarter)
            late_out[part, :] = (
                other[part, :] + term(j, left[:, i * quarter : (i + 1) * quarter], 1 - core)
            ).astype(BF16)
            go(late_copy(k))
        part = slice(h * hw, (h + 1) * hw)
        total_own[part, :] = total_own[part, :] + term(j, left, core)
        squares(j, h)

    def last_sub():
        for q in range(freqs):
            square = acc[q]
            lo, hi = q * 2 * vecs, (q * 2 + 1) * vecs
            sub_out[lo : lo + vecs, :] = (square[0:vecs, 0:vecs] + square[vecs:, vecs:]) * inv_grid
            sub_out[hi : hi + vecs, :] = (square[0:vecs, vecs:] - square[vecs:, 0:vecs]) * inv_grid
        go(sub_copy())

    def store(k):
        part = pl.ds(k * quarter, quarter)
        return pltpu.make_async_copy(total_own.at[part], images.at[part], sem_out.at[k])

    def last_add(k):
        late_copy(k).wait_recv()
        part = slice(k * quarter, (k + 1) * quarter)
        total_own[part, :] = total_own[part, :] + late_in[part, :].astype(F32)
        store(k).start()

    def last_wait():
        sub_copy().wait_recv()
        sub[...] = sub_out[...] + sub_in[...]
        for k in range(4):
            store(k).wait()

    one, two, rest = (1,), range(2, 3), range(3, chips)
    own = (0,)
    pack(0)
    pack(1)
    pack(2)
    pack(3)
    ready()
    exchange(0)
    for c in range(chunks):
        own_send(c)
    energies()
    vectors_send()
    relay(0, own)
    relay(1, own)
    spread(0, one)
    exchange(1)
    relay(2, own)
    spread(0, two)
    relay(3, own)
    spread(0, rest)
    relay(0, one)
    spread(1, one)
    relay(0, two)
    spread(1, two)
    exchange(2)
    relay(0, rest)
    spread(1, rest)
    pass_deltas()
    vectors()
    relay(1, one)
    spread(2, one)
    relay(1, two)
    spread(2, two)
    exchange(3)
    cross(0, 0)
    cross(0, 1)
    relay(1, rest)
    spread(2, rest)
    relay(2, one)
    spread(3, one)
    relay(2, two)
    spread(3, two)
    relay(2, rest)
    spread(3, rest)
    cross(1, 0)
    cross(1, 1)
    columns()
    scale(0, 0)
    scale(0, 1)
    relay(3, one)
    relay(3, two)
    cross(2, 0)
    cross(2, 1)
    relay(3, rest)
    scale(1, 0)
    scale(1, 1)
    share(0, 0)
    image(0, 0)
    image(0, 1)
    cross(3, 0)
    cross(3, 1)
    scale(2, 0)
    scale(2, 1)
    share(1, 0)
    image(1, 0)
    image(1, 1)
    scale(3, 0)
    scale(3, 1)
    share(2, 0)
    image(2, 0)
    image(2, 1)
    share(3, 0)
    last_other(0)
    share(3, 1)
    last_other(1)
    last_sub()
    last_add(0)
    last_add(1)
    last_add(2)
    last_add(3)
    last_wait()
    for copy in sends:
        copy.wait_send()


def shards(pair_density, trial_vectors, frequency, val_energy, cond_energy, pair_index):
    groups = lax.axis_size("freq")
    members = lax.axis_size("band")
    rows = pair_density.shape[0]
    freqs, _, vecs, grid_here = trial_vectors.shape
    pair_count = rows * groups * members
    grid_count = grid_here * members
    prefactor = 1.0 / math.sqrt(2.0 * grid_count * pair_count)
    width = freqs * 2 * vecs
    chips = members // 2
    chunks = rows // 8
    piece = rows // chunks
    slot = groups * piece
    wide = 2 * grid_here
    trial = trial_vectors.reshape(width, grid_here)
    dma = pltpu.SemaphoreType.DMA
    vmem = pl.BlockSpec(memory_space=pltpu.VMEM)
    anywhere = pl.BlockSpec(memory_space=pl.ANY)
    smem = pl.BlockSpec(memory_space=pltpu.SMEM)
    images, sub = pl.pallas_call(
        functools.partial(
            kernel, groups, members, chunks, freqs, vecs, rows, grid_here, prefactor, 1.0 / grid_count
        ),
        out_shape=(
            jax.ShapeDtypeStruct((width, grid_here), F32),
            jax.ShapeDtypeStruct((width, vecs), F32),
        ),
        in_specs=[anywhere] * 2 + [smem] * 3 + [vmem],
        out_specs=(anywhere, vmem),
        scratch_shapes=[
            pltpu.VMEM((rows, 2, grid_count), BF16),
            pltpu.VMEM((chunks, 2 * piece, grid_count), BF16),
            pltpu.VMEM((width, grid_here), F32),
            pltpu.VMEM((chunks, groups, chips, 2 * piece, wide), BF16),
            pltpu.VMEM((width, wide), BF16),
            pltpu.VMEM((8, 128), F32),
            pltpu.VMEM((1, width), F32),
            pltpu.VMEM((groups, chips, 8, 128), F32),
            pltpu.VMEM((chunks, chips * slot, 8), F32),
            pltpu.VMEM((chunks, 2, chips, slot, width // 2), BF16),
            pltpu.VMEM((chunks, 2, chips, slot, width // 2), BF16),
            pltpu.VMEM((chunks, 2, chips, slot, width // 2), BF16),
            pltpu.VMEM((freqs, 2 * vecs, 2 * vecs), F32),
            pltpu.VMEM((width, grid_here), F32),
            pltpu.VMEM((width, grid_here), BF16),
            pltpu.VMEM((width, grid_here), BF16),
            pltpu.VMEM((width, vecs), F32),
            pltpu.VMEM((width, vecs), F32),
            dma((chunks,)), dma((4,)),
            dma((chunks, chips)), dma((chunks, chips)),
            dma((2,)), dma((1,)),
            dma((chunks, groups, chips)), dma((chunks, groups, chips)),
            dma((chips,)), dma((chips,)),
            dma((groups,)), dma((groups,)),
            dma((chunks, 2, chips)), dma((chunks, 2, chips)),
            dma((chunks, 2, chips)), dma((chunks, 2, chips)),
            dma((5,)), dma((5,)),
        ],
        compiler_params=pltpu.CompilerParams(
            collective_id=0, has_side_effects=True, vmem_limit_bytes=56 * 1024 * 1024
        ),
    )(pair_density, trial, frequency, val_energy, cond_energy, pair_index[None, :])
    return (
        images.reshape(freqs, 2, vecs, grid_here),
        sub.reshape(freqs, 2, vecs, vecs),
    )


def solution(mesh):
    return jax.shard_map(
        shards,
        mesh=mesh,
        in_specs=(
            P(("freq", "band"), None, None),
            P("freq", None, None, "band"),
            P("freq"),
            P(),
            P(),
            P(("freq", "band")),
        ),
        out_specs=(P("freq", None, None, "band"), P("freq", None, None, None)),
        check_vma=False,
    )
```

```python
import functools
import math

import jax
import jax.numpy as jnp
from jax import lax
from jax.experimental import pallas as pl
from jax.experimental.pallas import tpu as pltpu
from jax.sharding import PartitionSpec as P

MESH = pl.DeviceIdType.MESH
F32 = jnp.float32
BF16 = jnp.bfloat16


def scoped(
    groups, members, chunks, freqs, vecs, rows, grid_here, prefactor, inv_grid,
    dens, trial, frequency_in, val_in, cond_in, index_in,
    total_out, sub_mine, sub_in,
    frequency, val_energy, cond_energy, pair_index,
    raw, packed, total_own, held, both, delta_own, freq_row, deltas, cols, ring_out, ring_in, scaled, acc,
    sub_out, held_p, scaled_p,
    sem_in, sem_out, sem_as, sem_ar, sem_os, sem_or, sem_fs, sem_fr, sem_ds, sem_dr, sem_es, sem_er,
    sem_rs, sem_rr, sem_gs, sem_gr, sem_ls, sem_lr, sem_qs, sem_qr, sem_is, sem_ir,
):
    f = lax.axis_index("freq")
    b = lax.axis_index("band")
    chips = members // 2
    piece = rows // chunks
    zc = b // 2
    core = b % 2
    width = freqs * 2 * vecs
    slot = groups * piece
    chunk_rows = chips * slot
    wide = 2 * grid_here
    partner = zc * 2 + (1 - core)

    def remote(src, dst, send, recv, freq_id, band_id):
        return pltpu.make_async_remote_copy(
            src_ref=src, dst_ref=dst, send_sem=send, recv_sem=recv,
            device_id=(freq_id, band_id), device_id_type=MESH,
        )

    def peer(s):
        return (zc + s) % chips * 2 + core

    barrier = pltpu.get_barrier_semaphore()
    pl.semaphore_signal(barrier, inc=1, device_id=(f, partner), device_id_type=MESH)
    for s in range(1, chips):
        pl.semaphore_signal(barrier, inc=1, device_id=(f, peer(s)), device_id_type=MESH)
    for s in range(1, groups):
        pl.semaphore_signal(barrier, inc=1, device_id=((f + s) % groups, b), device_id_type=MESH)

    def load(c):
        return pltpu.make_async_copy(
            dens.at[pl.ds(c * piece, piece)], raw.at[pl.ds(c * piece, piece)], sem_in.at[c]
        )

    for c in range(chunks):
        load(c).start()
    small = [
        pltpu.make_async_copy(src, dst, sem_in.at[chunks + i])
        for i, (src, dst) in enumerate(
            ((frequency_in, frequency), (val_in, val_energy), (cond_in, cond_energy), (index_in, pair_index))
        )
    ]
    for copy in small:
        copy.start()
    pltpu.make_async_copy(trial, both.at[:, pl.ds(pl.multiple_of(core * grid_here, 128), grid_here)], sem_os.at[1]).start()

    def pack(c):
        load(c).wait()
        packed[c] = jnp.swapaxes(raw[c * piece : (c + 1) * piece], 0, 1).reshape(2 * piece, -1)

    def ready():
        pl.semaphore_wait(barrier, chips + groups - 1)

    def waves(c, z):
        return packed.at[c, :, pl.ds(pl.multiple_of(z * wide, 128), wide)]

    sends = []

    def go(copy):
        copy.start()
        sends.append(copy)

    def exchange(c):
        for r in range(1, chips):
            z = (zc + r) % chips
            go(remote(waves(c, z), held.at[c, f, zc], sem_as.at[c, r], sem_ar.at[c, zc], f, peer(r)))

    square_groups = groups == 4
    xx, yy = f % 2, f // 2
    fx, fy = yy * 2 + (1 - xx), (1 - yy) * 2 + xx
    fd = (1 - yy) * 2 + (1 - xx)

    def piece_copy(c, g, z, lane, to):
        ref = held.at[c, g, z]
        return remote(ref, ref, sem_fs.at[c, lane, z], sem_fr.at[c, lane, z], to, b)

    def whole(c, g, lane, to):
        return remote(held.at[c, g], held.at[c, g], sem_fs.at[c, lane, 0], sem_fr.at[c, lane, 0], to, b)

    def own_send(c):
        keep = pltpu.make_async_copy(waves(c, zc), held.at[c, f, zc], sem_ar.at[c, zc])
        keep.start()
        if square_groups:
            for lane, to in ((0, fx), (1, fy)):
                go(remote(waves(c, zc), held.at[c, f, zc], sem_fs.at[c, lane, zc], sem_fr.at[c, lane, zc], to, b))

    def landed(c, z):
        pltpu.make_async_copy(waves(c, 0), held.at[c, f, z], sem_ar.at[c, z]).wait()

    def spread(c, offsets):
        for r in offsets:
            z = (zc + r) % chips
            landed(c, z)
            if square_groups:
                go(piece_copy(c, f, z, 0, fx))
                go(piece_copy(c, f, z, 1, fy))
        if not square_groups and offsets and offsets[-1] == chips - 1:
            landed(c, zc)
            for s in range(1, groups):
                go(whole(c, f, s, (f + s) % groups))

    def relay(c, offsets):
        if square_groups:
            for r in offsets:
                z = (zc + r) % chips
                if (r + c) % 2 == 0:
                    piece_copy(c, fx, z, 0, fx).wait_recv()
                    go(piece_copy(c, fx, z, 2, fy))
                else:
                    piece_copy(c, fy, z, 1, fy).wait_recv()
                    go(piece_copy(c, fy, z, 3, fx))

    def arrive(c):
        if square_groups:
            landed(c, zc)
            for r in range(chips):
                z = (zc + r) % chips
                if (r + c) % 2 == 0:
                    piece_copy(c, fy, z, 1, fy).wait_recv()
                    piece_copy(c, fd, z, 2, fy).wait_recv()
                else:
                    piece_copy(c, fx, z, 0, fx).wait_recv()
                    piece_copy(c, fd, z, 3, fx).wait_recv()
        else:
            for s in range(1, groups):
                src = (f + groups - s) % groups
                whole(c, src, s, src).wait_recv()

    def half_of(ref, k):
        return ref.at[:, pl.ds(pl.multiple_of(k * grid_here, 128), grid_here)]

    def vectors_send():
        go(remote(trial, half_of(both, core), sem_os.at[0], sem_or.at[0], f, partner))

    def vectors():
        pltpu.make_async_copy(trial, half_of(both, core), sem_os.at[1]).wait()
        remote(trial, half_of(both, 1 - core), sem_os.at[0], sem_or.at[0], f, partner).wait_recv()

    def energies():
        for copy in small:
            copy.wait()
        cond_count = cond_energy.shape[0]
        val_count = val_energy.shape[0]
        index = pair_index[...]
        rest_index = index
        val_pick = jnp.full(index.shape, val_energy[0], F32)
        for v in range(1, val_count):
            above = index >= v * cond_count
            val_pick = jnp.where(above, val_energy[v], val_pick)
            rest_index = jnp.where(above, index - v * cond_count, rest_index)
        cond_pick = jnp.full(index.shape, cond_energy[0], F32)
        for v in range(1, cond_count):
            cond_pick = jnp.where(rest_index == v, cond_energy[v], cond_pick)
        delta_own[...] = jnp.ones_like(delta_own)
        delta_own[0:1, 0:rows] = cond_pick - val_pick
        for q in range(freqs):
            freq_row[:, q * 2 * vecs : (q + 1) * 2 * vecs] = jnp.full((1, 2 * vecs), frequency[q], F32)
        pltpu.make_async_copy(delta_own, deltas.at[f, zc], sem_dr.at[zc]).start()
        for s in range(1, chips):
            go(remote(delta_own, deltas.at[f, zc], sem_ds.at[s], sem_dr.at[zc], f, peer(s)))

    def pass_deltas():
        for j in range(chips):
            pltpu.make_async_copy(delta_own, deltas.at[f, j], sem_dr.at[j]).wait()
        for s in range(1, groups):
            go(remote(deltas.at[f], deltas.at[f], sem_es.at[s], sem_er.at[s], (f + s) % groups, b))

    def columns():
        for s in range(1, groups):
            src = (f + groups - s) % groups
            remote(deltas.at[src], deltas.at[src], sem_es.at[s], sem_er.at[s], src, b).wait_recv()
        for g in range(groups):
            for j in range(chips):
                turned = jnp.transpose(deltas[g, j])
                at = (g * chips + j) * piece
                for c in range(chunks):
                    cols[c, at : at + piece, :] = turned[c * piece : (c + 1) * piece, :]

    hw = width // 2

    def weights(column, h):
        freq = freq_row[:, h * hw : (h + 1) * hw]
        ratio = column / (column * column + freq * freq)
        return (-4.0 * prefactor * ratio).astype(BF16).astype(F32)

    lane_at = lax.broadcasted_iota(jnp.int32, (1, 2 * vecs), 1)

    def swap(x, low, high):
        sign = jnp.where(lane_at < vecs, low, high)
        return jnp.concatenate(
            [
                pltpu.roll(x[:, q * 2 * vecs : (q + 1) * 2 * vecs], vecs, 1) * sign
                for q in range(freqs // 2)
            ],
            axis=1,
        )

    def lend(j):
        return remote(
            held.at[j, :, :, :, pl.ds(pl.multiple_of((1 - core) * grid_here, 128), grid_here)],
            held_p.at[j], sem_ls.at[j], sem_lr.at[j], f, partner,
        )

    def scaled_lend(j, h):
        if split(j):
            src, dst = scaled.at[j, h], scaled_p.at[j, h]
        else:
            src, dst, h = scaled.at[j], scaled_p.at[j], 0
        return remote(src, dst, sem_qs.at[j, h], sem_qr.at[j, h], f, partner)

    def cross(j):
        arrive(j)
        go(lend(j))
        over_grid = (((1,), (1,)), ((), ()))
        out = lax.dot_general(
            held[j].reshape(2 * chunk_rows, wide), both[...], over_grid, preferred_element_type=F32
        ).reshape(groups * chips, 2, piece, width)
        for h in range(2):
            part = slice(h * hw, (h + 1) * hw)
            total = out[:, 0, :, part].reshape(chunk_rows, hw) + swap(
                out[:, 1, :, part].reshape(chunk_rows, hw), 1.0, -1.0
            )
            ring_out[j, h] = total.astype(BF16).reshape(chips, slot, hw)
            if split(j) or h == 1:
                for s in range(1, chips):
                    go(slot_copy(j, h, s, (zc + s) % chips))

    def split(j):
        return j == chunks - 1

    def slot_copy(j, h, s, at):
        if split(j):
            src, dst = ring_out.at[j, h, at], ring_in.at[j, h, s]
        else:
            src, dst, h = ring_out.at[j, :, at], ring_in.at[j, :, s], 0
        return remote(src, dst, sem_rs.at[j, h, s], sem_rr.at[j, h, s], f, peer(s))

    def scaled_copy(j, h, s, at):
        if split(j):
            ref = scaled.at[j, h, at]
        else:
            ref, h = scaled.at[j, :, at], 0
        return remote(ref, ref, sem_gs.at[j, h, s], sem_gr.at[j, h, s], f, peer(s))

    def scale(j, h):
        total = ring_out[j, h, zc].astype(F32)
        for s in range(1, chips):
            if split(j) or h == 0:
                slot_copy(j, h, s, zc).wait_recv()
            total = total + ring_in[j, h, s].astype(F32)
        column = cols[j, pl.ds(pl.multiple_of(zc * slot, 8), slot), 0:1]
        scaled[j, h, zc] = (weights(column, h) * total).astype(BF16)
        if split(j) or h == 1:
            for s in range(1, chips):
                go(scaled_copy(j, h, s, zc))

    def share(j, h):
        if split(j) or h == 0:
            for s in range(1, chips):
                scaled_copy(j, h, s, (zc + chips - s) % chips).wait_recv()
            go(scaled_lend(j, h))

    over_rows = (((0,), (0,)), ((), ()))

    def paired(block):
        flat32 = block.reshape(chunk_rows, hw).astype(F32)
        turned = swap(flat32, -1.0, 1.0)
        return jnp.concatenate(
            [
                flat32.reshape(groups * chips, 1, piece, hw),
                turned.reshape(groups * chips, 1, piece, hw),
            ],
            axis=1,
        ).reshape(2 * chunk_rows, hw).astype(BF16)

    def add(j, h, term):
        part = slice(h * hw, (h + 1) * hw)
        if j == 0:
            total_own[part, :] = term
        else:
            total_own[part, :] = total_own[part, :] + term

    def here(j, h):
        right = held[j, :, :, :, pl.ds(pl.multiple_of(core * grid_here, 128), grid_here)]
        return lax.dot_general(
            paired(scaled[j, h]),
            right.reshape(2 * chunk_rows, grid_here),
            over_rows,
            preferred_element_type=F32,
        )

    def lent(j, h):
        if h == 0:
            lend(j).wait_recv()
        if split(j) or h == 0:
            scaled_lend(j, h).wait_recv()
        return lax.dot_general(
            paired(scaled_p[j, h]),
            held_p[j].reshape(2 * chunk_rows, grid_here),
            over_rows,
            preferred_element_type=F32,
        )

    def squares(j, h):
        flat = scaled[j, h].reshape(chunk_rows, hw)
        column = cols[j, :, 0:1]
        crossing = (flat.astype(F32) / weights(column, h)).astype(BF16)
        for i in range(freqs // 2):
            lo, hi = i * 2 * vecs, (i + 1) * 2 * vecs
            q = h * (freqs // 2) + i
            square = lax.dot_general(
                crossing[:, lo:hi], flat[:, lo:hi], over_rows, preferred_element_type=F32
            )
            if j == 0:
                acc[q] = square
            else:
                acc[q] = acc[q] + square

    def image(j, h):
        add(j, h, here(j, h) + lent(j, h))

    def last_own(h):
        add(chunks - 1, h, here(chunks - 1, h))

    def last_lent(h):
        add(chunks - 1, h, lent(chunks - 1, h))
        store(h).start()

    def sub_copy():
        return remote(sub_out, sub_in, sem_is.at[0], sem_ir.at[0], f, partner)

    def sub_keep():
        return pltpu.make_async_copy(sub_out, sub_mine, sem_out.at[2])

    def last_sub():
        for q in range(freqs):
            square = acc[q]
            lo, hi = q * 2 * vecs, (q * 2 + 1) * vecs
            sub_out[lo : lo + vecs, :] = (square[0:vecs, 0:vecs] + square[vecs:, vecs:]) * inv_grid
            sub_out[hi : hi + vecs, :] = (square[0:vecs, vecs:] - square[vecs:, 0:vecs]) * inv_grid
        go(sub_copy())
        sub_keep().start()

    def store(h):
        part = pl.ds(h * hw, hw)
        return pltpu.make_async_copy(total_own.at[part], total_out.at[part], sem_out.at[h])

    def last_wait():
        for h in range(2):
            store(h).wait()
        sub_keep().wait()
        sub_copy().wait_recv()

    one, two, rest = (1,), range(2, 3), range(3, chips)
    own = (0,)
    pack(0)
    pack(1)
    pack(2)
    pack(3)
    ready()
    exchange(0)
    for c in range(chunks):
        own_send(c)
    energies()
    vectors_send()
    relay(0, own)
    relay(1, own)
    spread(0, one)
    exchange(1)
    relay(2, own)
    spread(0, two)
    relay(3, own)
    spread(0, rest)
    relay(0, one)
    spread(1, one)
    relay(0, two)
    spread(1, two)
    exchange(2)
    relay(0, rest)
    spread(1, rest)
    pass_deltas()
    vectors()
    relay(1, one)
    spread(2, one)
    relay(1, two)
    spread(2, two)
    exchange(3)
    cross(0)
    relay(1, rest)
    spread(2, rest)
    relay(2, one)
    spread(3, one)
    relay(2, two)
    spread(3, two)
    relay(2, rest)
    spread(3, rest)
    cross(1)
    columns()
    scale(0, 0)
    scale(0, 1)
    relay(3, one)
    relay(3, two)
    cross(2)
    relay(3, rest)
    scale(1, 0)
    scale(1, 1)
    share(0, 0)
    squares(0, 0)
    squares(0, 1)
    cross(3)
    scale(2, 0)
    scale(2, 1)
    image(0, 0)
    image(0, 1)
    share(1, 0)
    squares(1, 0)
    squares(1, 1)
    scale(3, 0)
    scale(3, 1)
    image(1, 0)
    image(1, 1)
    share(2, 0)
    squares(2, 0)
    squares(2, 1)
    image(2, 0)
    image(2, 1)
    share(3, 0)
    last_own(0)
    squares(3, 0)
    share(3, 1)
    squares(3, 1)
    last_sub()
    last_own(1)
    last_lent(0)
    last_lent(1)
    last_wait()
    for copy in sends:
        copy.wait_send()


def kernel(statics, semaphores, *refs):
    pl.run_scoped(functools.partial(scoped, *statics, *refs), *semaphores)


def closing(total, sub_mine, sub_in, images, sub, total_v, sub_v, sub_iv, sem_a, sem_b, sem_c):
    blocks = sem_c.shape[0] - 1
    size = total.shape[0] // blocks

    def into(k):
        part = pl.ds(k * size, size)
        return pltpu.make_async_copy(total.at[part], total_v.at[part], sem_a.at[k])

    def out(k):
        part = pl.ds(k * size, size)
        return pltpu.make_async_copy(total_v.at[part], images.at[part], sem_c.at[k])

    for k in range(blocks):
        into(k).start()
    edge = (
        pltpu.make_async_copy(sub_mine, sub_v, sem_b.at[0]),
        pltpu.make_async_copy(sub_in, sub_iv, sem_b.at[1]),
    )
    for copy in edge:
        copy.start()
    for k in range(blocks):
        into(k).wait()
        out(k).start()
    for copy in edge:
        copy.wait()
    sub_v[...] = sub_v[...] + sub_iv[...]
    last = pltpu.make_async_copy(sub_v, sub, sem_c.at[blocks])
    last.start()
    for k in range(blocks):
        out(k).wait()
    last.wait()


def shards(pair_density, trial_vectors, frequency, val_energy, cond_energy, pair_index):
    groups = lax.axis_size("freq")
    members = lax.axis_size("band")
    rows = pair_density.shape[0]
    freqs, _, vecs, grid_here = trial_vectors.shape
    pair_count = rows * groups * members
    grid_count = grid_here * members
    prefactor = 1.0 / math.sqrt(2.0 * grid_count * pair_count)
    width = freqs * 2 * vecs
    chips = members // 2
    chunks = rows // 8
    piece = rows // chunks
    slot = groups * piece
    wide = 2 * grid_here
    trial = trial_vectors.reshape(width, grid_here)
    dma = pltpu.SemaphoreType.DMA
    anywhere = pl.BlockSpec(memory_space=pl.ANY)
    statics = (groups, members, chunks, freqs, vecs, rows, grid_here, prefactor, 1.0 / grid_count)
    semaphores = (
        dma((chunks + 4,)), dma((3,)), dma((chunks, chips)), dma((chunks, chips)), dma((2,)), dma((1,)), dma((chunks, groups, chips)), dma((chunks, groups, chips)), dma((chips,)), dma((chips,)), dma((groups,)), dma((groups,)), dma((chunks, 2, chips)), dma((chunks, 2, chips)), dma((chunks, 2, chips)), dma((chunks, 2, chips)), dma((chunks,)), dma((chunks,)), dma((chunks, 2)), dma((chunks, 2)), dma((1,)), dma((1,)),
    )
    parts = pl.pallas_call(
        functools.partial(kernel, statics, semaphores),
        out_shape=(
            jax.ShapeDtypeStruct((width, grid_here), F32),
            jax.ShapeDtypeStruct((width, vecs), F32),
            jax.ShapeDtypeStruct((width, vecs), F32),
        ),
        in_specs=[anywhere] * 6,
        out_specs=(anywhere,) * 3,
        scratch_shapes=[
            pltpu.SMEM(frequency.shape, F32),
            pltpu.SMEM(val_energy.shape, F32),
            pltpu.SMEM(cond_energy.shape, F32),
            pltpu.VMEM((1, rows), jnp.int32),
            pltpu.VMEM((rows, 2, grid_count), BF16),
            pltpu.VMEM((chunks, 2 * piece, grid_count), BF16),
            pltpu.VMEM((width, grid_here), F32),
            pltpu.VMEM((chunks, groups, chips, 2 * piece, wide), BF16),
            pltpu.VMEM((width, wide), BF16),
            pltpu.VMEM((8, 128), F32),
            pltpu.VMEM((1, width), F32),
            pltpu.VMEM((groups, chips, 8, 128), F32),
            pltpu.VMEM((chunks, chips * slot, 8), F32),
            pltpu.VMEM((chunks, 2, chips, slot, width // 2), BF16),
            pltpu.VMEM((chunks, 2, chips, slot, width // 2), BF16),
            pltpu.VMEM((chunks, 2, chips, slot, width // 2), BF16),
            pltpu.VMEM((freqs, 2 * vecs, 2 * vecs), F32),
            pltpu.VMEM((width, vecs), F32),
            pltpu.VMEM((chunks, groups, chips, 2 * piece, grid_here), BF16),
            pltpu.VMEM((chunks, 2, chips, slot, width // 2), BF16),
        ],
        compiler_params=pltpu.CompilerParams(
            collective_id=0, has_side_effects=True, vmem_limit_bytes=56 * 1024 * 1024
        ),
    )(pair_density, trial, frequency, val_energy, cond_energy, pair_index[None, :])
    blocks = 4
    images, sub = pl.pallas_call(
        closing,
        out_shape=(
            jax.ShapeDtypeStruct((width, grid_here), F32),
            jax.ShapeDtypeStruct((width, vecs), F32),
        ),
        in_specs=[anywhere] * 3,
        out_specs=(anywhere,) * 2,
        scratch_shapes=[
            pltpu.VMEM((width, grid_here), F32),
            pltpu.VMEM((width, vecs), F32),
            pltpu.VMEM((width, vecs), F32),
            dma((blocks,)), dma((2,)), dma((blocks + 1,)),
        ],
    )(*parts)
    return (
        images.reshape(freqs, 2, vecs, grid_here),
        sub.reshape(freqs, 2, vecs, vecs),
    )


def solution(mesh):
    return jax.shard_map(
        shards,
        mesh=mesh,
        in_specs=(
            P(("freq", "band"), None, None),
            P("freq", None, None, "band"),
            P("freq"),
            P(),
            P(),
            P(("freq", "band")),
        ),
        out_specs=(P("freq", None, None, "band"), P("freq", None, None, None)),
        check_vma=False,
    )
```

```python
import functools
import math

import jax
import jax.numpy as jnp
from jax import lax
from jax.experimental import pallas as pl
from jax.experimental.pallas import tpu as pltpu
from jax.sharding import PartitionSpec as P

MESH = pl.DeviceIdType.MESH
F32 = jnp.float32
BF16 = jnp.bfloat16


def scoped(
    groups, members, chunks, freqs, vecs, rows, grid_here, prefactor, inv_grid,
    dens, trial, frequency_in, val_in, cond_in, index_in,
    total_own, sub_out, sub_in,
    frequency, val_energy, cond_energy, pair_index,
    raw, packed, held, both, delta_own, freq_row, deltas, cols, ring_out, ring_in, scaled, acc,
    held_p, scaled_p,
    sem_in, sem_as, sem_ar, sem_os, sem_or, sem_fs, sem_fr, sem_ds, sem_dr, sem_es, sem_er,
    sem_rs, sem_rr, sem_gs, sem_gr, sem_ls, sem_lr, sem_qs, sem_qr, sem_is, sem_ir,
):
    f = lax.axis_index("freq")
    b = lax.axis_index("band")
    chips = members // 2
    piece = rows // chunks
    zc = b // 2
    core = b % 2
    width = freqs * 2 * vecs
    slot = groups * piece
    chunk_rows = chips * slot
    wide = 2 * grid_here
    partner = zc * 2 + (1 - core)

    def remote(src, dst, send, recv, freq_id, band_id):
        return pltpu.make_async_remote_copy(
            src_ref=src, dst_ref=dst, send_sem=send, recv_sem=recv,
            device_id=(freq_id, band_id), device_id_type=MESH,
        )

    def peer(s):
        return (zc + s) % chips * 2 + core

    barrier = pltpu.get_barrier_semaphore()
    pl.semaphore_signal(barrier, inc=1, device_id=(f, partner), device_id_type=MESH)
    for s in range(1, chips):
        pl.semaphore_signal(barrier, inc=1, device_id=(f, peer(s)), device_id_type=MESH)
    for s in range(1, groups):
        pl.semaphore_signal(barrier, inc=1, device_id=((f + s) % groups, b), device_id_type=MESH)

    def load(c):
        return pltpu.make_async_copy(
            dens.at[pl.ds(c * piece, piece)], raw.at[pl.ds(c * piece, piece)], sem_in.at[c]
        )

    for c in range(chunks):
        load(c).start()
    small = [
        pltpu.make_async_copy(src, dst, sem_in.at[chunks + i])
        for i, (src, dst) in enumerate(
            ((frequency_in, frequency), (val_in, val_energy), (cond_in, cond_energy), (index_in, pair_index))
        )
    ]
    for copy in small:
        copy.start()
    pltpu.make_async_copy(trial, both.at[:, pl.ds(pl.multiple_of(core * grid_here, 128), grid_here)], sem_os.at[1]).start()

    def pack(c):
        load(c).wait()
        packed[c] = jnp.swapaxes(raw[c * piece : (c + 1) * piece], 0, 1).reshape(2 * piece, -1)

    def ready():
        pl.semaphore_wait(barrier, chips + groups - 1)

    def waves(c, z):
        return packed.at[c, :, pl.ds(pl.multiple_of(z * wide, 128), wide)]

    sends = []

    def go(copy):
        copy.start()
        sends.append(copy)

    def exchange(c):
        for r in range(1, chips):
            z = (zc + r) % chips
            go(remote(waves(c, z), held.at[c, f, zc], sem_as.at[c, r], sem_ar.at[c, zc], f, peer(r)))

    square_groups = groups == 4
    xx, yy = f % 2, f // 2
    fx, fy = yy * 2 + (1 - xx), (1 - yy) * 2 + xx
    fd = (1 - yy) * 2 + (1 - xx)

    def piece_copy(c, g, z, lane, to):
        ref = held.at[c, g, z]
        return remote(ref, ref, sem_fs.at[c, lane, z], sem_fr.at[c, lane, z], to, b)

    def whole(c, g, lane, to):
        return remote(held.at[c, g], held.at[c, g], sem_fs.at[c, lane, 0], sem_fr.at[c, lane, 0], to, b)

    def own_send(c):
        keep = pltpu.make_async_copy(waves(c, zc), held.at[c, f, zc], sem_ar.at[c, zc])
        keep.start()
        if square_groups:
            for lane, to in ((0, fx), (1, fy)):
                go(remote(waves(c, zc), held.at[c, f, zc], sem_fs.at[c, lane, zc], sem_fr.at[c, lane, zc], to, b))

    def landed(c, z):
        pltpu.make_async_copy(waves(c, 0), held.at[c, f, z], sem_ar.at[c, z]).wait()

    def spread(c, offsets):
        for r in offsets:
            z = (zc + r) % chips
            landed(c, z)
            if square_groups:
                go(piece_copy(c, f, z, 0, fx))
                go(piece_copy(c, f, z, 1, fy))
        if not square_groups and offsets and offsets[-1] == chips - 1:
            landed(c, zc)
            for s in range(1, groups):
                go(whole(c, f, s, (f + s) % groups))

    def relay(c, offsets):
        if square_groups:
            for r in offsets:
                z = (zc + r) % chips
                if (r + c) % 2 == 0:
                    piece_copy(c, fx, z, 0, fx).wait_recv()
                    go(piece_copy(c, fx, z, 2, fy))
                else:
                    piece_copy(c, fy, z, 1, fy).wait_recv()
                    go(piece_copy(c, fy, z, 3, fx))

    def arrive(c):
        if square_groups:
            landed(c, zc)
            for r in range(chips):
                z = (zc + r) % chips
                if (r + c) % 2 == 0:
                    piece_copy(c, fy, z, 1, fy).wait_recv()
                    piece_copy(c, fd, z, 2, fy).wait_recv()
                else:
                    piece_copy(c, fx, z, 0, fx).wait_recv()
                    piece_copy(c, fd, z, 3, fx).wait_recv()
        else:
            for s in range(1, groups):
                src = (f + groups - s) % groups
                whole(c, src, s, src).wait_recv()

    def half_of(ref, k):
        return ref.at[:, pl.ds(pl.multiple_of(k * grid_here, 128), grid_here)]

    def vectors_send():
        go(remote(trial, half_of(both, core), sem_os.at[0], sem_or.at[0], f, partner))

    def vectors():
        pltpu.make_async_copy(trial, half_of(both, core), sem_os.at[1]).wait()
        remote(trial, half_of(both, 1 - core), sem_os.at[0], sem_or.at[0], f, partner).wait_recv()

    def energies():
        for copy in small:
            copy.wait()
        cond_count = cond_energy.shape[0]
        val_count = val_energy.shape[0]
        index = pair_index[...]
        rest_index = index
        val_pick = jnp.full(index.shape, val_energy[0], F32)
        for v in range(1, val_count):
            above = index >= v * cond_count
            val_pick = jnp.where(above, val_energy[v], val_pick)
            rest_index = jnp.where(above, index - v * cond_count, rest_index)
        cond_pick = jnp.full(index.shape, cond_energy[0], F32)
        for v in range(1, cond_count):
            cond_pick = jnp.where(rest_index == v, cond_energy[v], cond_pick)
        delta_own[...] = jnp.ones_like(delta_own)
        delta_own[0:1, 0:rows] = cond_pick - val_pick
        for q in range(freqs):
            freq_row[:, q * 2 * vecs : (q + 1) * 2 * vecs] = jnp.full((1, 2 * vecs), frequency[q], F32)
        pltpu.make_async_copy(delta_own, deltas.at[f, zc], sem_dr.at[zc]).start()
        for s in range(1, chips):
            go(remote(delta_own, deltas.at[f, zc], sem_ds.at[s], sem_dr.at[zc], f, peer(s)))

    def pass_deltas():
        for j in range(chips):
            pltpu.make_async_copy(delta_own, deltas.at[f, j], sem_dr.at[j]).wait()
        for s in range(1, groups):
            go(remote(deltas.at[f], deltas.at[f], sem_es.at[s], sem_er.at[s], (f + s) % groups, b))

    def columns():
        for s in range(1, groups):
            src = (f + groups - s) % groups
            remote(deltas.at[src], deltas.at[src], sem_es.at[s], sem_er.at[s], src, b).wait_recv()
        for g in range(groups):
            for j in range(chips):
                turned = jnp.transpose(deltas[g, j])
                at = (g * chips + j) * piece
                for c in range(chunks):
                    cols[c, at : at + piece, :] = turned[c * piece : (c + 1) * piece, :]

    hw = width // 2

    def weights(column, h):
        freq = freq_row[:, h * hw : (h + 1) * hw]
        ratio = column / (column * column + freq * freq)
        return (-4.0 * prefactor * ratio).astype(BF16).astype(F32)

    lane_at = lax.broadcasted_iota(jnp.int32, (1, 2 * vecs), 1)

    def swap(x, low, high):
        sign = jnp.where(lane_at < vecs, low, high)
        return jnp.concatenate(
            [
                pltpu.roll(x[:, q * 2 * vecs : (q + 1) * 2 * vecs], vecs, 1) * sign
                for q in range(freqs // 2)
            ],
            axis=1,
        )

    def lend(j):
        return remote(
            held.at[j, :, :, :, pl.ds(pl.multiple_of((1 - core) * grid_here, 128), grid_here)],
            held_p.at[j], sem_ls.at[j], sem_lr.at[j], f, partner,
        )

    def scaled_lend(j, h):
        if split(j):
            src, dst = scaled.at[j, h], scaled_p.at[j, h]
        else:
            src, dst, h = scaled.at[j], scaled_p.at[j], 0
        return remote(src, dst, sem_qs.at[j, h], sem_qr.at[j, h], f, partner)

    def cross(j):
        arrive(j)
        go(lend(j))
        over_grid = (((1,), (1,)), ((), ()))
        out = lax.dot_general(
            held[j].reshape(2 * chunk_rows, wide), both[...], over_grid, preferred_element_type=F32
        ).reshape(groups * chips, 2, piece, width)
        for h in range(2):
            part = slice(h * hw, (h + 1) * hw)
            total = out[:, 0, :, part].reshape(chunk_rows, hw) + swap(
                out[:, 1, :, part].reshape(chunk_rows, hw), 1.0, -1.0
            )
            ring_out[j, h] = total.astype(BF16).reshape(chips, slot, hw)
            if split(j) or h == 1:
                for s in range(1, chips):
                    go(slot_copy(j, h, s, (zc + s) % chips))

    def split(j):
        return j == chunks - 1

    def slot_copy(j, h, s, at):
        if split(j):
            src, dst = ring_out.at[j, h, at], ring_in.at[j, h, s]
        else:
            src, dst, h = ring_out.at[j, :, at], ring_in.at[j, :, s], 0
        return remote(src, dst, sem_rs.at[j, h, s], sem_rr.at[j, h, s], f, peer(s))

    def scaled_copy(j, h, s, at):
        if split(j):
            ref = scaled.at[j, h, at]
        else:
            ref, h = scaled.at[j, :, at], 0
        return remote(ref, ref, sem_gs.at[j, h, s], sem_gr.at[j, h, s], f, peer(s))

    def scale(j, h):
        total = ring_out[j, h, zc].astype(F32)
        for s in range(1, chips):
            if split(j) or h == 0:
                slot_copy(j, h, s, zc).wait_recv()
            total = total + ring_in[j, h, s].astype(F32)
        column = cols[j, pl.ds(pl.multiple_of(zc * slot, 8), slot), 0:1]
        scaled[j, h, zc] = (weights(column, h) * total).astype(BF16)
        if split(j) or h == 1:
            for s in range(1, chips):
                go(scaled_copy(j, h, s, zc))

    def share(j, h):
        if split(j) or h == 0:
            for s in range(1, chips):
                scaled_copy(j, h, s, (zc + chips - s) % chips).wait_recv()
            go(scaled_lend(j, h))

    over_rows = (((0,), (0,)), ((), ()))

    def paired(block):
        flat32 = block.reshape(chunk_rows, hw).astype(F32)
        turned = swap(flat32, -1.0, 1.0)
        return jnp.concatenate(
            [
                flat32.reshape(groups * chips, 1, piece, hw),
                turned.reshape(groups * chips, 1, piece, hw),
            ],
            axis=1,
        ).reshape(2 * chunk_rows, hw).astype(BF16)

    def add(j, h, term):
        part = slice(h * hw, (h + 1) * hw)
        if j == 0:
            total_own[part, :] = term
        else:
            total_own[part, :] = total_own[part, :] + term

    def here(j, h):
        right = held[j, :, :, :, pl.ds(pl.multiple_of(core * grid_here, 128), grid_here)]
        return lax.dot_general(
            paired(scaled[j, h]),
            right.reshape(2 * chunk_rows, grid_here),
            over_rows,
            preferred_element_type=F32,
        )

    def lent(j, h):
        if h == 0:
            lend(j).wait_recv()
        if split(j) or h == 0:
            scaled_lend(j, h).wait_recv()
        return lax.dot_general(
            paired(scaled_p[j, h]),
            held_p[j].reshape(2 * chunk_rows, grid_here),
            over_rows,
            preferred_element_type=F32,
        )

    def squares(j, h):
        flat = scaled[j, h].reshape(chunk_rows, hw)
        column = cols[j, :, 0:1]
        crossing = (flat.astype(F32) / weights(column, h)).astype(BF16)
        for i in range(freqs // 2):
            lo, hi = i * 2 * vecs, (i + 1) * 2 * vecs
            q = h * (freqs // 2) + i
            square = lax.dot_general(
                crossing[:, lo:hi], flat[:, lo:hi], over_rows, preferred_element_type=F32
            )
            if j == 0:
                acc[q] = square
            else:
                acc[q] = acc[q] + square

    def image(j, h):
        add(j, h, here(j, h) + lent(j, h))

    def last_own(h):
        add(chunks - 1, h, here(chunks - 1, h))

    def last_lent(h):
        add(chunks - 1, h, lent(chunks - 1, h))

    def sub_copy():
        return remote(sub_out, sub_in, sem_is.at[0], sem_ir.at[0], f, partner)

    def last_sub():
        for q in range(freqs):
            square = acc[q]
            lo, hi = q * 2 * vecs, (q * 2 + 1) * vecs
            sub_out[lo : lo + vecs, :] = (square[0:vecs, 0:vecs] + square[vecs:, vecs:]) * inv_grid
            sub_out[hi : hi + vecs, :] = (square[0:vecs, vecs:] - square[vecs:, 0:vecs]) * inv_grid
        go(sub_copy())

    def last_wait():
        sub_copy().wait_recv()

    one, two, rest = (1,), range(2, 3), range(3, chips)
    own = (0,)
    pack(0)
    pack(1)
    pack(2)
    pack(3)
    ready()
    exchange(0)
    for c in range(chunks):
        own_send(c)
    energies()
    vectors_send()
    relay(0, own)
    relay(1, own)
    spread(0, one)
    exchange(1)
    relay(2, own)
    spread(0, two)
    relay(3, own)
    spread(0, rest)
    relay(0, one)
    spread(1, one)
    relay(0, two)
    spread(1, two)
    exchange(2)
    relay(0, rest)
    spread(1, rest)
    pass_deltas()
    vectors()
    relay(1, one)
    relay(1, two)
    spread(2, one)
    spread(2, two)
    exchange(3)
    cross(0)
    relay(1, rest)
    spread(2, rest)
    relay(2, one)
    spread(3, one)
    relay(2, two)
    spread(3, two)
    relay(2, rest)
    columns()
    spread(3, rest)
    cross(1)
    scale(0, 0)
    scale(0, 1)
    relay(3, one)
    relay(3, two)
    cross(2)
    scale(1, 0)
    scale(1, 1)
    share(0, 0)
    squares(0, 0)
    squares(0, 1)
    relay(3, rest)
    cross(3)
    scale(2, 0)
    scale(2, 1)
    image(0, 0)
    image(0, 1)
    share(1, 0)
    squares(1, 0)
    squares(1, 1)
    scale(3, 0)
    scale(3, 1)
    image(1, 0)
    image(1, 1)
    share(2, 0)
    squares(2, 0)
    squares(2, 1)
    image(2, 0)
    image(2, 1)
    share(3, 0)
    last_own(0)
    squares(3, 0)
    share(3, 1)
    squares(3, 1)
    last_sub()
    last_own(1)
    last_lent(0)
    last_lent(1)
    last_wait()
    for copy in sends:
        copy.wait_send()


def kernel(statics, semaphores, *refs):
    pl.run_scoped(functools.partial(scoped, *statics, *refs), *semaphores)


def closing(total, sub_mine, sub_in, images, sub, sub_v):
    def run(sem):
        copy = pltpu.make_async_copy(total, images, sem.at[0])
        copy.start()
        sub_v[...] = sub_mine[...] + sub_in[...]
        edge = pltpu.make_async_copy(sub_v, sub, sem.at[1])
        edge.start()
        copy.wait()
        edge.wait()

    pl.run_scoped(run, pltpu.SemaphoreType.DMA((2,)))


def shards(pair_density, trial_vectors, frequency, val_energy, cond_energy, pair_index):
    groups = lax.axis_size("freq")
    members = lax.axis_size("band")
    rows = pair_density.shape[0]
    freqs, _, vecs, grid_here = trial_vectors.shape
    pair_count = rows * groups * members
    grid_count = grid_here * members
    prefactor = 1.0 / math.sqrt(2.0 * grid_count * pair_count)
    width = freqs * 2 * vecs
    chips = members // 2
    chunks = rows // 8
    piece = rows // chunks
    slot = groups * piece
    wide = 2 * grid_here
    trial = trial_vectors.reshape(width, grid_here)
    dma = pltpu.SemaphoreType.DMA
    vmem = pl.BlockSpec(memory_space=pltpu.VMEM)
    anywhere = pl.BlockSpec(memory_space=pl.ANY)
    statics = (groups, members, chunks, freqs, vecs, rows, grid_here, prefactor, 1.0 / grid_count)
    semaphores = (
        dma((chunks + 4,)), dma((chunks, chips)), dma((chunks, chips)), dma((2,)), dma((1,)), dma((chunks, groups, chips)), dma((chunks, groups, chips)), dma((chips,)), dma((chips,)), dma((groups,)), dma((groups,)), dma((chunks, 2, chips)), dma((chunks, 2, chips)), dma((chunks, 2, chips)), dma((chunks, 2, chips)), dma((chunks,)), dma((chunks,)), dma((chunks, 2)), dma((chunks, 2)), dma((1,)), dma((1,)),
    )
    parts = pl.pallas_call(
        functools.partial(kernel, statics, semaphores),
        out_shape=(
            pltpu.VMEM((width, grid_here), F32),
            pltpu.VMEM((width, vecs), F32),
            pltpu.VMEM((width, vecs), F32),
        ),
        in_specs=[anywhere] * 6,
        out_specs=(vmem,) * 3,
        scratch_shapes=[
            pltpu.SMEM(frequency.shape, F32),
            pltpu.SMEM(val_energy.shape, F32),
            pltpu.SMEM(cond_energy.shape, F32),
            pltpu.VMEM((1, rows), jnp.int32),
            pltpu.VMEM((rows, 2, grid_count), BF16),
            pltpu.VMEM((chunks, 2 * piece, grid_count), BF16),
            pltpu.VMEM((chunks, groups, chips, 2 * piece, wide), BF16),
            pltpu.VMEM((width, wide), BF16),
            pltpu.VMEM((8, 128), F32),
            pltpu.VMEM((1, width), F32),
            pltpu.VMEM((groups, chips, 8, 128), F32),
            pltpu.VMEM((chunks, chips * slot, 8), F32),
            pltpu.VMEM((chunks, 2, chips, slot, width // 2), BF16),
            pltpu.VMEM((chunks, 2, chips, slot, width // 2), BF16),
            pltpu.VMEM((chunks, 2, chips, slot, width // 2), BF16),
            pltpu.VMEM((freqs, 2 * vecs, 2 * vecs), F32),
            pltpu.VMEM((chunks, groups, chips, 2 * piece, grid_here), BF16),
            pltpu.VMEM((chunks, 2, chips, slot, width // 2), BF16),
        ],
        compiler_params=pltpu.CompilerParams(
            collective_id=0, has_side_effects=True, vmem_limit_bytes=40 * 1024 * 1024
        ),
    )(
        *(
            pltpu.with_memory_space_constraint(x, pltpu.HBM)
            for x in (pair_density, trial, frequency, val_energy, cond_energy, pair_index[None, :])
        )
    )
    images, sub = pl.pallas_call(
        closing,
        out_shape=(
            jax.ShapeDtypeStruct((width, grid_here), F32),
            jax.ShapeDtypeStruct((width, vecs), F32),
        ),
        in_specs=[vmem] * 3,
        out_specs=(anywhere,) * 2,
        scratch_shapes=[pltpu.VMEM((width, vecs), F32)],
        compiler_params=pltpu.CompilerParams(vmem_limit_bytes=16 * 1024 * 1024),
    )(*(pltpu.with_memory_space_constraint(x, pltpu.VMEM) for x in parts))
    return (
        images.reshape(freqs, 2, vecs, grid_here),
        sub.reshape(freqs, 2, vecs, vecs),
    )


def solution(mesh):
    return jax.shard_map(
        shards,
        mesh=mesh,
        in_specs=(
            P(("freq", "band"), None, None),
            P("freq", None, None, "band"),
            P("freq"),
            P(),
            P(),
            P(("freq", "band")),
        ),
        out_specs=(P("freq", None, None, "band"), P("freq", None, None, None)),
        check_vma=False,
    )
```

```python
import functools
import math

import jax
import jax.numpy as jnp
from jax import lax
from jax.experimental import pallas as pl
from jax.experimental.pallas import tpu as pltpu
from jax.sharding import PartitionSpec as P

MESH = pl.DeviceIdType.MESH
F32 = jnp.float32
BF16 = jnp.bfloat16


def scoped(
    groups, members, chunks, freqs, vecs, rows, grid_here, prefactor, inv_grid,
    dens, trial, frequency_in, val_in, cond_in, index_in,
    total_own, sub_out, sub_in,
    frequency, val_energy, cond_energy, pair_index,
    raw, packed, held, both, delta_own, freq_row, deltas, cols, ring_out, ring_in, scaled, acc,
    held_p, scaled_p,
    sem_in, sem_as, sem_ar, sem_os, sem_or, sem_fs, sem_fr, sem_ds, sem_dr, sem_es, sem_er,
    sem_rs, sem_rr, sem_gs, sem_gr, sem_ls, sem_lr, sem_qs, sem_qr, sem_is, sem_ir,
):
    f = lax.axis_index("freq")
    b = lax.axis_index("band")
    chips = members // 2
    piece = rows // chunks
    zc = b // 2
    core = b % 2
    width = freqs * 2 * vecs
    slot = groups * piece
    chunk_rows = chips * slot
    wide = 2 * grid_here
    partner = zc * 2 + (1 - core)

    def remote(src, dst, send, recv, freq_id, band_id):
        return pltpu.make_async_remote_copy(
            src_ref=src, dst_ref=dst, send_sem=send, recv_sem=recv,
            device_id=(freq_id, band_id), device_id_type=MESH,
        )

    def peer(s):
        return (zc + s) % chips * 2 + core

    barrier = pltpu.get_barrier_semaphore()
    pl.semaphore_signal(barrier, inc=1, device_id=(f, partner), device_id_type=MESH)
    for s in range(1, chips):
        pl.semaphore_signal(barrier, inc=1, device_id=(f, peer(s)), device_id_type=MESH)
    for s in range(1, groups):
        pl.semaphore_signal(barrier, inc=1, device_id=((f + s) % groups, b), device_id_type=MESH)

    def load(c):
        return pltpu.make_async_copy(
            dens.at[pl.ds(c * piece, piece)], raw.at[pl.ds(c * piece, piece)], sem_in.at[c]
        )

    for c in range(chunks):
        load(c).start()
    small = [
        pltpu.make_async_copy(src, dst, sem_in.at[chunks + i])
        for i, (src, dst) in enumerate(
            ((frequency_in, frequency), (val_in, val_energy), (cond_in, cond_energy), (index_in, pair_index))
        )
    ]
    for copy in small:
        copy.start()
    pltpu.make_async_copy(trial, both.at[:, pl.ds(pl.multiple_of(core * grid_here, 128), grid_here)], sem_os.at[1]).start()

    def pack(c):
        load(c).wait()
        packed[c] = jnp.swapaxes(raw[c * piece : (c + 1) * piece], 0, 1).reshape(2 * piece, -1)

    def ready():
        pl.semaphore_wait(barrier, chips + groups - 1)

    def waves(c, z):
        return packed.at[c, :, pl.ds(pl.multiple_of(z * wide, 128), wide)]

    sends = []

    def go(copy):
        copy.start()
        sends.append(copy)

    def exchange(c):
        for r in range(1, chips):
            z = (zc + r) % chips
            go(remote(waves(c, z), held.at[c, f, zc], sem_as.at[c, r], sem_ar.at[c, zc], f, peer(r)))

    square_groups = groups == 4
    xx, yy = f % 2, f // 2
    fx, fy = yy * 2 + (1 - xx), (1 - yy) * 2 + xx
    fd = (1 - yy) * 2 + (1 - xx)

    def piece_copy(c, g, z, lane, to):
        ref = held.at[c, g, z]
        return remote(ref, ref, sem_fs.at[c, lane, z], sem_fr.at[c, lane, z], to, b)

    def whole(c, g, lane, to):
        return remote(held.at[c, g], held.at[c, g], sem_fs.at[c, lane, 0], sem_fr.at[c, lane, 0], to, b)

    def own_send(c):
        keep = pltpu.make_async_copy(waves(c, zc), held.at[c, f, zc], sem_ar.at[c, zc])
        keep.start()
        if square_groups:
            for lane, to in ((0, fx), (1, fy)):
                go(remote(waves(c, zc), held.at[c, f, zc], sem_fs.at[c, lane, zc], sem_fr.at[c, lane, zc], to, b))

    def landed(c, z):
        pltpu.make_async_copy(waves(c, 0), held.at[c, f, z], sem_ar.at[c, z]).wait()

    def spread(c, offsets):
        for r in offsets:
            z = (zc + r) % chips
            landed(c, z)
            if square_groups:
                go(piece_copy(c, f, z, 0, fx))
                go(piece_copy(c, f, z, 1, fy))
        if not square_groups and offsets and offsets[-1] == chips - 1:
            landed(c, zc)
            for s in range(1, groups):
                go(whole(c, f, s, (f + s) % groups))

    def relay(c, offsets):
        if square_groups:
            for r in offsets:
                z = (zc + r) % chips
                if (r + c) % 2 == 0:
                    piece_copy(c, fx, z, 0, fx).wait_recv()
                    go(piece_copy(c, fx, z, 2, fy))
                else:
                    piece_copy(c, fy, z, 1, fy).wait_recv()
                    go(piece_copy(c, fy, z, 3, fx))

    def arrive(c):
        if square_groups:
            landed(c, zc)
            for r in range(chips):
                z = (zc + r) % chips
                if (r + c) % 2 == 0:
                    piece_copy(c, fy, z, 1, fy).wait_recv()
                    piece_copy(c, fd, z, 2, fy).wait_recv()
                else:
                    piece_copy(c, fx, z, 0, fx).wait_recv()
                    piece_copy(c, fd, z, 3, fx).wait_recv()
        else:
            for s in range(1, groups):
                src = (f + groups - s) % groups
                whole(c, src, s, src).wait_recv()

    def half_of(ref, k):
        return ref.at[:, pl.ds(pl.multiple_of(k * grid_here, 128), grid_here)]

    def vectors_send():
        go(remote(trial, half_of(both, core), sem_os.at[0], sem_or.at[0], f, partner))

    def vectors():
        pltpu.make_async_copy(trial, half_of(both, core), sem_os.at[1]).wait()
        remote(trial, half_of(both, 1 - core), sem_os.at[0], sem_or.at[0], f, partner).wait_recv()

    def energies():
        for copy in small:
            copy.wait()
        cond_count = cond_energy.shape[0]
        val_count = val_energy.shape[0]
        index = pair_index[...]
        rest_index = index
        val_pick = jnp.full(index.shape, val_energy[0], F32)
        for v in range(1, val_count):
            above = index >= v * cond_count
            val_pick = jnp.where(above, val_energy[v], val_pick)
            rest_index = jnp.where(above, index - v * cond_count, rest_index)
        cond_pick = jnp.full(index.shape, cond_energy[0], F32)
        for v in range(1, cond_count):
            cond_pick = jnp.where(rest_index == v, cond_energy[v], cond_pick)
        delta_own[...] = jnp.ones_like(delta_own)
        delta_own[0:1, 0:rows] = cond_pick - val_pick
        for q in range(freqs):
            freq_row[:, q * 2 * vecs : (q + 1) * 2 * vecs] = jnp.full((1, 2 * vecs), frequency[q], F32)
        pltpu.make_async_copy(delta_own, deltas.at[f, zc], sem_dr.at[zc]).start()
        for s in range(1, chips):
            go(remote(delta_own, deltas.at[f, zc], sem_ds.at[s], sem_dr.at[zc], f, peer(s)))

    def pass_deltas():
        for j in range(chips):
            pltpu.make_async_copy(delta_own, deltas.at[f, j], sem_dr.at[j]).wait()
        for s in range(1, groups):
            go(remote(deltas.at[f], deltas.at[f], sem_es.at[s], sem_er.at[s], (f + s) % groups, b))

    def columns():
        for s in range(1, groups):
            src = (f + groups - s) % groups
            remote(deltas.at[src], deltas.at[src], sem_es.at[s], sem_er.at[s], src, b).wait_recv()
        for g in range(groups):
            for j in range(chips):
                turned = jnp.transpose(deltas[g, j])
                at = (g * chips + j) * piece
                for c in range(chunks):
                    cols[c, at : at + piece, :] = turned[c * piece : (c + 1) * piece, :]

    hw = width // 2

    def weights(column, h):
        freq = freq_row[:, h * hw : (h + 1) * hw]
        ratio = column / (column * column + freq * freq)
        return (-4.0 * prefactor * ratio).astype(BF16).astype(F32)

    lane_at = lax.broadcasted_iota(jnp.int32, (1, 2 * vecs), 1)

    def swap(x, low, high):
        sign = jnp.where(lane_at < vecs, low, high)
        return jnp.concatenate(
            [
                pltpu.roll(x[:, q * 2 * vecs : (q + 1) * 2 * vecs], vecs, 1) * sign
                for q in range(freqs // 2)
            ],
            axis=1,
        )

    def lend(j):
        return remote(
            held.at[j, :, :, :, pl.ds(pl.multiple_of((1 - core) * grid_here, 128), grid_here)],
            held_p.at[j], sem_ls.at[j], sem_lr.at[j], f, partner,
        )

    def scaled_lend(j, h):
        if split(j):
            src, dst = scaled.at[j, h], scaled_p.at[j, h]
        else:
            src, dst, h = scaled.at[j], scaled_p.at[j], 0
        return remote(src, dst, sem_qs.at[j, h], sem_qr.at[j, h], f, partner)

    def cross(j):
        arrive(j)
        over_grid = (((1,), (1,)), ((), ()))
        out = lax.dot_general(
            held[j].reshape(2 * chunk_rows, wide), both[...], over_grid, preferred_element_type=F32
        ).reshape(groups * chips, 2, piece, width)
        for h in range(2):
            part = slice(h * hw, (h + 1) * hw)
            total = out[:, 0, :, part].reshape(chunk_rows, hw) + swap(
                out[:, 1, :, part].reshape(chunk_rows, hw), 1.0, -1.0
            )
            ring_out[j, h] = total.astype(BF16).reshape(chips, slot, hw)
            if split(j) or h == 1:
                for s in range(1, chips):
                    go(slot_copy(j, h, s, (zc + s) % chips))
        go(lend(j))

    def split(j):
        return j == chunks - 1

    def slot_copy(j, h, s, at):
        if split(j):
            src, dst = ring_out.at[j, h, at], ring_in.at[j, h, s]
        else:
            src, dst, h = ring_out.at[j, :, at], ring_in.at[j, :, s], 0
        return remote(src, dst, sem_rs.at[j, h, s], sem_rr.at[j, h, s], f, peer(s))

    def scaled_copy(j, h, s, at):
        if split(j):
            ref = scaled.at[j, h, at]
        else:
            ref, h = scaled.at[j, :, at], 0
        return remote(ref, ref, sem_gs.at[j, h, s], sem_gr.at[j, h, s], f, peer(s))

    def scale(j, h):
        total = ring_out[j, h, zc].astype(F32)
        for s in range(1, chips):
            if split(j) or h == 0:
                slot_copy(j, h, s, zc).wait_recv()
            total = total + ring_in[j, h, s].astype(F32)
        column = cols[j, pl.ds(pl.multiple_of(zc * slot, 8), slot), 0:1]
        scaled[j, h, zc] = (weights(column, h) * total).astype(BF16)
        if split(j) or h == 1:
            for s in range(1, chips):
                go(scaled_copy(j, h, s, zc))

    def share(j, h):
        if split(j) or h == 0:
            for s in range(1, chips):
                scaled_copy(j, h, s, (zc + chips - s) % chips).wait_recv()
            go(scaled_lend(j, h))

    over_rows = (((0,), (0,)), ((), ()))

    def paired(block):
        flat32 = block.reshape(chunk_rows, hw).astype(F32)
        turned = swap(flat32, -1.0, 1.0)
        return jnp.concatenate(
            [
                flat32.reshape(groups * chips, 1, piece, hw),
                turned.reshape(groups * chips, 1, piece, hw),
            ],
            axis=1,
        ).reshape(2 * chunk_rows, hw).astype(BF16)

    def add(j, h, term):
        part = slice(h * hw, (h + 1) * hw)
        if j == 0:
            total_own[part, :] = term
        else:
            total_own[part, :] = total_own[part, :] + term

    def here(j, h):
        right = held[j, :, :, :, pl.ds(pl.multiple_of(core * grid_here, 128), grid_here)]
        return lax.dot_general(
            paired(scaled[j, h]),
            right.reshape(2 * chunk_rows, grid_here),
            over_rows,
            preferred_element_type=F32,
        )

    def lent(j, h):
        if h == 0:
            lend(j).wait_recv()
        if split(j) or h == 0:
            scaled_lend(j, h).wait_recv()
        return lax.dot_general(
            paired(scaled_p[j, h]),
            held_p[j].reshape(2 * chunk_rows, grid_here),
            over_rows,
            preferred_element_type=F32,
        )

    def squares(j, h):
        flat = scaled[j, h].reshape(chunk_rows, hw)
        column = cols[j, :, 0:1]
        crossing = (flat.astype(F32) / weights(column, h)).astype(BF16)
        for i in range(freqs // 2):
            lo, hi = i * 2 * vecs, (i + 1) * 2 * vecs
            q = h * (freqs // 2) + i
            square = lax.dot_general(
                crossing[:, lo:hi], flat[:, lo:hi], over_rows, preferred_element_type=F32
            )
            if j == 0:
                acc[q] = square
            else:
                acc[q] = acc[q] + square

    def image(j, h):
        add(j, h, here(j, h) + lent(j, h))

    def own_term(j, h):
        add(j, h, here(j, h))

    def lent_term(j, h):
        add(j, h, lent(j, h))

    def last_own(h):
        add(chunks - 1, h, here(chunks - 1, h))

    def last_lent(h):
        add(chunks - 1, h, lent(chunks - 1, h))

    def sub_copy():
        return remote(sub_out, sub_in, sem_is.at[0], sem_ir.at[0], f, partner)

    def last_sub():
        for q in range(freqs):
            square = acc[q]
            lo, hi = q * 2 * vecs, (q * 2 + 1) * vecs
            sub_out[lo : lo + vecs, :] = (square[0:vecs, 0:vecs] + square[vecs:, vecs:]) * inv_grid
            sub_out[hi : hi + vecs, :] = (square[0:vecs, vecs:] - square[vecs:, 0:vecs]) * inv_grid
        go(sub_copy())

    def last_wait():
        sub_copy().wait_recv()

    one, two, rest = (1,), range(2, 3), range(3, chips)
    own = (0,)
    pack(0)
    pack(1)
    pack(2)
    pack(3)
    ready()
    exchange(0)
    for c in range(chunks):
        own_send(c)
    energies()
    relay(0, own)
    relay(1, own)
    spread(0, one)
    relay(2, own)
    spread(0, two)
    exchange(1)
    relay(3, own)
    spread(0, rest)
    vectors_send()
    relay(0, one)
    spread(1, one)
    relay(0, two)
    spread(1, two)
    exchange(2)
    relay(0, rest)
    spread(1, rest)
    pass_deltas()
    vectors()
    relay(1, one)
    relay(1, two)
    spread(2, one)
    spread(2, two)
    exchange(3)
    cross(0)
    relay(1, rest)
    spread(2, rest)
    relay(2, one)
    spread(3, one)
    relay(2, two)
    spread(3, two)
    relay(2, rest)
    columns()
    spread(3, rest)
    cross(1)
    scale(0, 0)
    scale(0, 1)
    relay(3, one)
    relay(3, two)
    cross(2)
    scale(1, 0)
    scale(1, 1)
    relay(3, rest)
    share(0, 0)
    squares(0, 0)
    squares(0, 1)
    cross(3)
    scale(2, 0)
    scale(2, 1)
    image(0, 0)
    image(0, 1)
    share(1, 0)
    squares(1, 0)
    squares(1, 1)
    scale(3, 0)
    scale(3, 1)
    image(1, 0)
    image(1, 1)
    share(2, 0)
    squares(2, 0)
    squares(2, 1)
    own_term(2, 0)
    own_term(2, 1)
    share(3, 0)
    own_term(3, 0)
    squares(3, 0)
    share(3, 1)
    squares(3, 1)
    last_sub()
    own_term(3, 1)
    lent_term(2, 0)
    lent_term(2, 1)
    last_lent(0)
    last_lent(1)
    last_wait()
    for copy in sends:
        copy.wait_send()


def kernel(statics, semaphores, *refs):
    pl.run_scoped(functools.partial(scoped, *statics, *refs), *semaphores)


def closing(total, sub_mine, sub_in, images, sub, sub_v):
    def run(sem):
        size = total.shape[0] // 4
        copies = [
            pltpu.make_async_copy(total.at[pl.ds(k * size, size)], images.at[pl.ds(k * size, size)], sem.at[2 + k])
            for k in range(4)
        ]
        for copy in copies:
            copy.start()
        sub_v[...] = sub_mine[...] + sub_in[...]
        edge = pltpu.make_async_copy(sub_v, sub, sem.at[1])
        edge.start()
        for copy in copies:
            copy.wait()
        edge.wait()

    pl.run_scoped(run, pltpu.SemaphoreType.DMA((6,)))


def shards(pair_density, trial_vectors, frequency, val_energy, cond_energy, pair_index):
    groups = lax.axis_size("freq")
    members = lax.axis_size("band")
    rows = pair_density.shape[0]
    freqs, _, vecs, grid_here = trial_vectors.shape
    pair_count = rows * groups * members
    grid_count = grid_here * members
    prefactor = 1.0 / math.sqrt(2.0 * grid_count * pair_count)
    width = freqs * 2 * vecs
    chips = members // 2
    chunks = rows // 8
    piece = rows // chunks
    slot = groups * piece
    wide = 2 * grid_here
    trial = trial_vectors.reshape(width, grid_here)
    dma = pltpu.SemaphoreType.DMA
    vmem = pl.BlockSpec(memory_space=pltpu.VMEM)
    anywhere = pl.BlockSpec(memory_space=pl.ANY)
    statics = (groups, members, chunks, freqs, vecs, rows, grid_here, prefactor, 1.0 / grid_count)
    semaphores = (
        dma((chunks + 4,)), dma((chunks, chips)), dma((chunks, chips)), dma((2,)), dma((1,)), dma((chunks, groups, chips)), dma((chunks, groups, chips)), dma((chips,)), dma((chips,)), dma((groups,)), dma((groups,)), dma((chunks, 2, chips)), dma((chunks, 2, chips)), dma((chunks, 2, chips)), dma((chunks, 2, chips)), dma((chunks,)), dma((chunks,)), dma((chunks, 2)), dma((chunks, 2)), dma((1,)), dma((1,)),
    )
    parts = pl.pallas_call(
        functools.partial(kernel, statics, semaphores),
        out_shape=(
            pltpu.VMEM((width, grid_here), F32),
            pltpu.VMEM((width, vecs), F32),
            pltpu.VMEM((width, vecs), F32),
        ),
        in_specs=[anywhere] * 6,
        out_specs=(vmem,) * 3,
        scratch_shapes=[
            pltpu.SMEM(frequency.shape, F32),
            pltpu.SMEM(val_energy.shape, F32),
            pltpu.SMEM(cond_energy.shape, F32),
            pltpu.VMEM((1, rows), jnp.int32),
            pltpu.VMEM((rows, 2, grid_count), BF16),
            pltpu.VMEM((chunks, 2 * piece, grid_count), BF16),
            pltpu.VMEM((chunks, groups, chips, 2 * piece, wide), BF16),
            pltpu.VMEM((width, wide), BF16),
            pltpu.VMEM((8, 128), F32),
            pltpu.VMEM((1, width), F32),
            pltpu.VMEM((groups, chips, 8, 128), F32),
            pltpu.VMEM((chunks, chips * slot, 8), F32),
            pltpu.VMEM((chunks, 2, chips, slot, width // 2), BF16),
            pltpu.VMEM((chunks, 2, chips, slot, width // 2), BF16),
            pltpu.VMEM((chunks, 2, chips, slot, width // 2), BF16),
            pltpu.VMEM((freqs, 2 * vecs, 2 * vecs), F32),
            pltpu.VMEM((chunks, groups, chips, 2 * piece, grid_here), BF16),
            pltpu.VMEM((chunks, 2, chips, slot, width // 2), BF16),
        ],
        compiler_params=pltpu.CompilerParams(
            collective_id=0, has_side_effects=True, vmem_limit_bytes=40 * 1024 * 1024
        ),
    )(
        *(
            pltpu.with_memory_space_constraint(x, pltpu.HBM)
            for x in (pair_density, trial, frequency, val_energy, cond_energy, pair_index[None, :])
        )
    )
    images, sub = pl.pallas_call(
        closing,
        out_shape=(
            jax.ShapeDtypeStruct((width, grid_here), F32),
            jax.ShapeDtypeStruct((width, vecs), F32),
        ),
        in_specs=[vmem] * 3,
        out_specs=(anywhere,) * 2,
        scratch_shapes=[pltpu.VMEM((width, vecs), F32)],
        compiler_params=pltpu.CompilerParams(vmem_limit_bytes=16 * 1024 * 1024),
    )(*(pltpu.with_memory_space_constraint(x, pltpu.VMEM) for x in parts))
    return (
        images.reshape(freqs, 2, vecs, grid_here),
        sub.reshape(freqs, 2, vecs, vecs),
    )


def solution(mesh):
    return jax.shard_map(
        shards,
        mesh=mesh,
        in_specs=(
            P(("freq", "band"), None, None),
            P("freq", None, None, "band"),
            P("freq"),
            P(),
            P(),
            P(("freq", "band")),
        ),
        out_specs=(P("freq", None, None, "band"), P("freq", None, None, None)),
        check_vma=False,
    )
```

```python
import functools
import math

import jax
import jax.numpy as jnp
from jax import lax
from jax.experimental import pallas as pl
from jax.experimental.pallas import tpu as pltpu
from jax.sharding import PartitionSpec as P

MESH = pl.DeviceIdType.MESH
F32 = jnp.float32
BF16 = jnp.bfloat16


def scoped(
    groups, members, chunks, freqs, vecs, rows, grid_here, prefactor, inv_grid,
    dens, trial, frequency_in, val_in, cond_in, index_in,
    total_own, sub_out, sub_in,
    frequency, val_energy, cond_energy, pair_index,
    raw, packed, held, both, delta_own, freq_row, deltas, cols, ring_out, ring_in, scaled, acc,
    held_p, scaled_p, inverse,
    sem_in, sem_as, sem_ar, sem_os, sem_or, sem_fs, sem_fr, sem_ds, sem_dr, sem_es, sem_er,
    sem_rs, sem_rr, sem_gs, sem_gr, sem_ls, sem_lr, sem_qs, sem_qr, sem_is, sem_ir,
):
    f = lax.axis_index("freq")
    b = lax.axis_index("band")
    chips = members // 2
    piece = rows // chunks
    zc = b // 2
    core = b % 2
    width = freqs * 2 * vecs
    slot = groups * piece
    chunk_rows = chips * slot
    wide = 2 * grid_here
    partner = zc * 2 + (1 - core)

    def remote(src, dst, send, recv, freq_id, band_id):
        return pltpu.make_async_remote_copy(
            src_ref=src, dst_ref=dst, send_sem=send, recv_sem=recv,
            device_id=(freq_id, band_id), device_id_type=MESH,
        )

    def peer(s):
        return (zc + s) % chips * 2 + core

    barrier = pltpu.get_barrier_semaphore()
    pl.semaphore_signal(barrier, inc=1, device_id=(f, partner), device_id_type=MESH)
    for s in range(1, chips):
        pl.semaphore_signal(barrier, inc=1, device_id=(f, peer(s)), device_id_type=MESH)
    for s in range(1, groups):
        pl.semaphore_signal(barrier, inc=1, device_id=((f + s) % groups, b), device_id_type=MESH)

    def load(c):
        return pltpu.make_async_copy(
            dens.at[pl.ds(c * piece, piece)], raw.at[pl.ds(c * piece, piece)], sem_in.at[c]
        )

    for c in range(chunks):
        load(c).start()
    small = [
        pltpu.make_async_copy(src, dst, sem_in.at[chunks + i])
        for i, (src, dst) in enumerate(
            ((frequency_in, frequency), (val_in, val_energy), (cond_in, cond_energy), (index_in, pair_index))
        )
    ]
    for copy in small:
        copy.start()
    pltpu.make_async_copy(trial, both.at[:, pl.ds(pl.multiple_of(core * grid_here, 128), grid_here)], sem_os.at[1]).start()

    def pack(c):
        load(c).wait()
        packed[c] = jnp.swapaxes(raw[c * piece : (c + 1) * piece], 0, 1).reshape(2 * piece, -1)

    def ready():
        pl.semaphore_wait(barrier, chips + groups - 1)

    def waves(c, z):
        return packed.at[c, :, pl.ds(pl.multiple_of(z * wide, 128), wide)]

    sends = []

    def go(copy):
        copy.start()
        sends.append(copy)

    def exchange(c):
        for r in range(1, chips):
            z = (zc + r) % chips
            go(remote(waves(c, z), held.at[c, f, zc], sem_as.at[c, r], sem_ar.at[c, zc], f, peer(r)))

    square_groups = groups == 4
    xx, yy = f % 2, f // 2
    fx, fy = yy * 2 + (1 - xx), (1 - yy) * 2 + xx
    fd = (1 - yy) * 2 + (1 - xx)

    def piece_copy(c, g, z, lane, to):
        ref = held.at[c, g, z]
        return remote(ref, ref, sem_fs.at[c, lane, z], sem_fr.at[c, lane, z], to, b)

    def whole(c, g, lane, to):
        return remote(held.at[c, g], held.at[c, g], sem_fs.at[c, lane, 0], sem_fr.at[c, lane, 0], to, b)

    def own_send(c):
        keep = pltpu.make_async_copy(waves(c, zc), held.at[c, f, zc], sem_ar.at[c, zc])
        keep.start()
        if square_groups:
            for lane, to in ((0, fx), (1, fy)):
                go(remote(waves(c, zc), held.at[c, f, zc], sem_fs.at[c, lane, zc], sem_fr.at[c, lane, zc], to, b))

    def landed(c, z):
        pltpu.make_async_copy(waves(c, 0), held.at[c, f, z], sem_ar.at[c, z]).wait()

    def spread(c, offsets):
        for r in offsets:
            z = (zc + r) % chips
            landed(c, z)
            if square_groups:
                go(piece_copy(c, f, z, 0, fx))
                go(piece_copy(c, f, z, 1, fy))
        if not square_groups and offsets and offsets[-1] == chips - 1:
            landed(c, zc)
            for s in range(1, groups):
                go(whole(c, f, s, (f + s) % groups))

    def relay(c, offsets):
        if square_groups:
            for r in offsets:
                z = (zc + r) % chips
                if (r + c) % 2 == 0:
                    piece_copy(c, fx, z, 0, fx).wait_recv()
                    go(piece_copy(c, fx, z, 2, fy))
                else:
                    piece_copy(c, fy, z, 1, fy).wait_recv()
                    go(piece_copy(c, fy, z, 3, fx))

    def arrive(c):
        if square_groups:
            landed(c, zc)
            for r in range(chips):
                z = (zc + r) % chips
                if (r + c) % 2 == 0:
                    piece_copy(c, fy, z, 1, fy).wait_recv()
                    piece_copy(c, fd, z, 2, fy).wait_recv()
                else:
                    piece_copy(c, fx, z, 0, fx).wait_recv()
                    piece_copy(c, fd, z, 3, fx).wait_recv()
        else:
            for s in range(1, groups):
                src = (f + groups - s) % groups
                whole(c, src, s, src).wait_recv()

    def half_of(ref, k):
        return ref.at[:, pl.ds(pl.multiple_of(k * grid_here, 128), grid_here)]

    def vectors_send():
        go(remote(trial, half_of(both, core), sem_os.at[0], sem_or.at[0], f, partner))

    def vectors():
        pltpu.make_async_copy(trial, half_of(both, core), sem_os.at[1]).wait()
        remote(trial, half_of(both, 1 - core), sem_os.at[0], sem_or.at[0], f, partner).wait_recv()

    def energies():
        for copy in small:
            copy.wait()
        cond_count = cond_energy.shape[0]
        val_count = val_energy.shape[0]
        index = pair_index[...]
        rest_index = index
        val_pick = jnp.full(index.shape, val_energy[0], F32)
        for v in range(1, val_count):
            above = index >= v * cond_count
            val_pick = jnp.where(above, val_energy[v], val_pick)
            rest_index = jnp.where(above, index - v * cond_count, rest_index)
        cond_pick = jnp.full(index.shape, cond_energy[0], F32)
        for v in range(1, cond_count):
            cond_pick = jnp.where(rest_index == v, cond_energy[v], cond_pick)
        delta_own[...] = jnp.ones_like(delta_own)
        delta_own[0:1, 0:rows] = cond_pick - val_pick
        for q in range(freqs):
            freq_row[:, q * 2 * vecs : (q + 1) * 2 * vecs] = jnp.full((1, 2 * vecs), frequency[q], F32)
        pltpu.make_async_copy(delta_own, deltas.at[f, zc], sem_dr.at[zc]).start()
        for s in range(1, chips):
            go(remote(delta_own, deltas.at[f, zc], sem_ds.at[s], sem_dr.at[zc], f, peer(s)))

    def pass_deltas():
        for j in range(chips):
            pltpu.make_async_copy(delta_own, deltas.at[f, j], sem_dr.at[j]).wait()
        for s in range(1, groups):
            go(remote(deltas.at[f], deltas.at[f], sem_es.at[s], sem_er.at[s], (f + s) % groups, b))

    def columns():
        for s in range(1, groups):
            src = (f + groups - s) % groups
            remote(deltas.at[src], deltas.at[src], sem_es.at[s], sem_er.at[s], src, b).wait_recv()
        for g in range(groups):
            for j in range(chips):
                turned = jnp.transpose(deltas[g, j])
                at = (g * chips + j) * piece
                for c in range(chunks):
                    cols[c, at : at + piece, :] = turned[c * piece : (c + 1) * piece, :]

    hw = width // 2

    def weights(column, h):
        freq = freq_row[:, h * hw : (h + 1) * hw]
        ratio = column / (column * column + freq * freq)
        return (-4.0 * prefactor * ratio).astype(BF16).astype(F32)

    lane_at = lax.broadcasted_iota(jnp.int32, (1, 2 * vecs), 1)

    def swap(x, low, high):
        sign = jnp.where(lane_at < vecs, low, high)
        return jnp.concatenate(
            [
                pltpu.roll(x[:, q * 2 * vecs : (q + 1) * 2 * vecs], vecs, 1) * sign
                for q in range(freqs // 2)
            ],
            axis=1,
        )

    def lend(j):
        return remote(
            held.at[j, :, :, :, pl.ds(pl.multiple_of((1 - core) * grid_here, 128), grid_here)],
            held_p.at[j], sem_ls.at[j], sem_lr.at[j], f, partner,
        )

    def scaled_lend(j, h):
        if split(j):
            src, dst = scaled.at[j, h], scaled_p.at[j, h]
        else:
            src, dst, h = scaled.at[j], scaled_p.at[j], 0
        return remote(src, dst, sem_qs.at[j, h], sem_qr.at[j, h], f, partner)

    def cross(j):
        arrive(j)
        over_grid = (((1,), (1,)), ((), ()))
        out = lax.dot_general(
            held[j].reshape(2 * chunk_rows, wide), both[...], over_grid, preferred_element_type=F32
        ).reshape(groups * chips, 2, piece, width)
        for h in range(2):
            part = slice(h * hw, (h + 1) * hw)
            total = out[:, 0, :, part].reshape(chunk_rows, hw) + swap(
                out[:, 1, :, part].reshape(chunk_rows, hw), 1.0, -1.0
            )
            ring_out[j, h] = total.astype(BF16).reshape(chips, slot, hw)
            if split(j) or h == 1:
                for s in range(1, chips):
                    go(slot_copy(j, h, s, (zc + s) % chips))
        go(lend(j))

    def split(j):
        return j == chunks - 1

    def slot_copy(j, h, s, at):
        if split(j):
            src, dst = ring_out.at[j, h, at], ring_in.at[j, h, s]
        else:
            src, dst, h = ring_out.at[j, :, at], ring_in.at[j, :, s], 0
        return remote(src, dst, sem_rs.at[j, h, s], sem_rr.at[j, h, s], f, peer(s))

    def scaled_copy(j, h, s, at):
        if split(j):
            ref = scaled.at[j, h, at]
        else:
            ref, h = scaled.at[j, :, at], 0
        return remote(ref, ref, sem_gs.at[j, h, s], sem_gr.at[j, h, s], f, peer(s))

    def scale(j, h):
        total = ring_out[j, h, zc].astype(F32)
        for s in range(1, chips):
            if split(j) or h == 0:
                slot_copy(j, h, s, zc).wait_recv()
            total = total + ring_in[j, h, s].astype(F32)
        column = cols[j, pl.ds(pl.multiple_of(zc * slot, 8), slot), 0:1]
        scaled[j, h, zc] = (weights(column, h) * total).astype(BF16)
        if split(j) or h == 1:
            for s in range(1, chips):
                go(scaled_copy(j, h, s, zc))

    def share(j, h):
        if split(j) or h == 0:
            for s in range(1, chips):
                scaled_copy(j, h, s, (zc + chips - s) % chips).wait_recv()
            go(scaled_lend(j, h))

    over_rows = (((0,), (0,)), ((), ()))

    def paired(block):
        flat32 = block.reshape(chunk_rows, hw).astype(F32)
        turned = swap(flat32, -1.0, 1.0)
        return jnp.concatenate(
            [
                flat32.reshape(groups * chips, 1, piece, hw),
                turned.reshape(groups * chips, 1, piece, hw),
            ],
            axis=1,
        ).reshape(2 * chunk_rows, hw).astype(BF16)

    def add(j, h, term):
        part = slice(h * hw, (h + 1) * hw)
        if j == 0:
            total_own[part, :] = term
        else:
            total_own[part, :] = total_own[part, :] + term

    def here(j, h):
        right = held[j, :, :, :, pl.ds(pl.multiple_of(core * grid_here, 128), grid_here)]
        return lax.dot_general(
            paired(scaled[j, h]),
            right.reshape(2 * chunk_rows, grid_here),
            over_rows,
            preferred_element_type=F32,
        )

    def lent(j, h):
        if h == 0:
            lend(j).wait_recv()
        if split(j) or h == 0:
            scaled_lend(j, h).wait_recv()
        return lax.dot_general(
            paired(scaled_p[j, h]),
            held_p[j].reshape(2 * chunk_rows, grid_here),
            over_rows,
            preferred_element_type=F32,
        )

    def invert():
        for h in range(2):
            inverse[h] = 1.0 / weights(cols[chunks - 1, :, 0:1], h)

    def squares(j, h):
        flat = scaled[j, h].reshape(chunk_rows, hw)
        if split(j):
            crossing = (flat.astype(F32) * inverse[h]).astype(BF16)
        else:
            column = cols[j, :, 0:1]
            crossing = (flat.astype(F32) / weights(column, h)).astype(BF16)
        for i in range(freqs // 2):
            lo, hi = i * 2 * vecs, (i + 1) * 2 * vecs
            q = h * (freqs // 2) + i
            square = lax.dot_general(
                crossing[:, lo:hi], flat[:, lo:hi], over_rows, preferred_element_type=F32
            )
            if j == 0:
                acc[q] = square
            else:
                acc[q] = acc[q] + square

    def image(j, h):
        add(j, h, here(j, h) + lent(j, h))

    def own_term(j, h):
        add(j, h, here(j, h))

    def lent_term(j, h):
        add(j, h, lent(j, h))

    def last_own(h):
        add(chunks - 1, h, here(chunks - 1, h))

    def last_lent(h):
        add(chunks - 1, h, lent(chunks - 1, h))

    def sub_copy():
        return remote(sub_out, sub_in, sem_is.at[0], sem_ir.at[0], f, partner)

    def last_sub():
        for q in range(freqs):
            square = acc[q]
            lo, hi = q * 2 * vecs, (q * 2 + 1) * vecs
            sub_out[lo : lo + vecs, :] = (square[0:vecs, 0:vecs] + square[vecs:, vecs:]) * inv_grid
            sub_out[hi : hi + vecs, :] = (square[0:vecs, vecs:] - square[vecs:, 0:vecs]) * inv_grid
        go(sub_copy())

    def last_wait():
        sub_copy().wait_recv()

    one, two, rest = (1,), range(2, 3), range(3, chips)
    own = (0,)
    pack(0)
    pack(1)
    pack(2)
    pack(3)
    ready()
    exchange(0)
    for c in range(chunks):
        own_send(c)
    energies()
    relay(0, own)
    relay(1, own)
    spread(0, one)
    relay(2, own)
    spread(0, two)
    exchange(1)
    relay(3, own)
    spread(0, rest)
    vectors_send()
    relay(0, one)
    spread(1, one)
    relay(0, two)
    spread(1, two)
    exchange(2)
    relay(0, rest)
    spread(1, rest)
    pass_deltas()
    vectors()
    relay(1, one)
    relay(1, two)
    spread(2, one)
    spread(2, two)
    exchange(3)
    cross(0)
    relay(1, rest)
    spread(2, rest)
    relay(2, one)
    spread(3, one)
    relay(2, two)
    spread(3, two)
    relay(2, rest)
    columns()
    spread(3, rest)
    cross(1)
    scale(0, 0)
    scale(0, 1)
    relay(3, one)
    relay(3, two)
    cross(2)
    scale(1, 0)
    scale(1, 1)
    relay(3, rest)
    share(0, 0)
    squares(0, 0)
    squares(0, 1)
    cross(3)
    scale(2, 0)
    scale(2, 1)
    image(0, 0)
    image(0, 1)
    invert()
    share(1, 0)
    squares(1, 0)
    squares(1, 1)
    scale(3, 0)
    scale(3, 1)
    image(1, 0)
    image(1, 1)
    share(2, 0)
    squares(2, 0)
    squares(2, 1)
    own_term(2, 0)
    own_term(2, 1)
    share(3, 0)
    own_term(3, 0)
    squares(3, 0)
    share(3, 1)
    squares(3, 1)
    last_sub()
    own_term(3, 1)
    lent_term(2, 0)
    lent_term(2, 1)
    last_lent(0)
    last_lent(1)
    last_wait()
    for copy in sends:
        copy.wait_send()


def kernel(statics, semaphores, *refs):
    pl.run_scoped(functools.partial(scoped, *statics, *refs), *semaphores)


def closing(total, sub_mine, sub_in, images, sub, sub_v):
    def run(sem):
        size = total.shape[0] // 4
        copies = [
            pltpu.make_async_copy(total.at[pl.ds(k * size, size)], images.at[pl.ds(k * size, size)], sem.at[2 + k])
            for k in range(4)
        ]
        for copy in copies:
            copy.start()
        sub_v[...] = sub_mine[...] + sub_in[...]
        edge = pltpu.make_async_copy(sub_v, sub, sem.at[1])
        edge.start()
        for copy in copies:
            copy.wait()
        edge.wait()

    pl.run_scoped(run, pltpu.SemaphoreType.DMA((6,)))


def shards(pair_density, trial_vectors, frequency, val_energy, cond_energy, pair_index):
    groups = lax.axis_size("freq")
    members = lax.axis_size("band")
    rows = pair_density.shape[0]
    freqs, _, vecs, grid_here = trial_vectors.shape
    pair_count = rows * groups * members
    grid_count = grid_here * members
    prefactor = 1.0 / math.sqrt(2.0 * grid_count * pair_count)
    width = freqs * 2 * vecs
    chips = members // 2
    chunks = rows // 8
    piece = rows // chunks
    slot = groups * piece
    wide = 2 * grid_here
    trial = trial_vectors.reshape(width, grid_here)
    dma = pltpu.SemaphoreType.DMA
    vmem = pl.BlockSpec(memory_space=pltpu.VMEM)
    anywhere = pl.BlockSpec(memory_space=pl.ANY)
    statics = (groups, members, chunks, freqs, vecs, rows, grid_here, prefactor, 1.0 / grid_count)
    semaphores = (
        dma((chunks + 4,)), dma((chunks, chips)), dma((chunks, chips)), dma((2,)), dma((1,)), dma((chunks, groups, chips)), dma((chunks, groups, chips)), dma((chips,)), dma((chips,)), dma((groups,)), dma((groups,)), dma((chunks, 2, chips)), dma((chunks, 2, chips)), dma((chunks, 2, chips)), dma((chunks, 2, chips)), dma((chunks,)), dma((chunks,)), dma((chunks, 2)), dma((chunks, 2)), dma((1,)), dma((1,)),
    )
    parts = pl.pallas_call(
        functools.partial(kernel, statics, semaphores),
        out_shape=(
            pltpu.VMEM((width, grid_here), F32),
            pltpu.VMEM((width, vecs), F32),
            pltpu.VMEM((width, vecs), F32),
        ),
        in_specs=[anywhere] * 6,
        out_specs=(vmem,) * 3,
        scratch_shapes=[
            pltpu.SMEM(frequency.shape, F32),
            pltpu.SMEM(val_energy.shape, F32),
            pltpu.SMEM(cond_energy.shape, F32),
            pltpu.VMEM((1, rows), jnp.int32),
            pltpu.VMEM((rows, 2, grid_count), BF16),
            pltpu.VMEM((chunks, 2 * piece, grid_count), BF16),
            pltpu.VMEM((chunks, groups, chips, 2 * piece, wide), BF16),
            pltpu.VMEM((width, wide), BF16),
            pltpu.VMEM((8, 128), F32),
            pltpu.VMEM((1, width), F32),
            pltpu.VMEM((groups, chips, 8, 128), F32),
            pltpu.VMEM((chunks, chips * slot, 8), F32),
            pltpu.VMEM((chunks, 2, chips, slot, width // 2), BF16),
            pltpu.VMEM((chunks, 2, chips, slot, width // 2), BF16),
            pltpu.VMEM((chunks, 2, chips, slot, width // 2), BF16),
            pltpu.VMEM((freqs, 2 * vecs, 2 * vecs), F32),
            pltpu.VMEM((chunks, groups, chips, 2 * piece, grid_here), BF16),
            pltpu.VMEM((chunks, 2, chips, slot, width // 2), BF16),
            pltpu.VMEM((2, chips * slot, width // 2), F32),
        ],
        compiler_params=pltpu.CompilerParams(
            collective_id=0, has_side_effects=True, vmem_limit_bytes=40 * 1024 * 1024
        ),
    )(
        *(
            pltpu.with_memory_space_constraint(x, pltpu.HBM)
            for x in (pair_density, trial, frequency, val_energy, cond_energy, pair_index[None, :])
        )
    )
    images, sub = pl.pallas_call(
        closing,
        out_shape=(
            jax.ShapeDtypeStruct((width, grid_here), F32),
            jax.ShapeDtypeStruct((width, vecs), F32),
        ),
        in_specs=[vmem] * 3,
        out_specs=(anywhere,) * 2,
        scratch_shapes=[pltpu.VMEM((width, vecs), F32)],
        compiler_params=pltpu.CompilerParams(vmem_limit_bytes=16 * 1024 * 1024),
    )(*(pltpu.with_memory_space_constraint(x, pltpu.VMEM) for x in parts))
    return (
        images.reshape(freqs, 2, vecs, grid_here),
        sub.reshape(freqs, 2, vecs, vecs),
    )


def solution(mesh):
    return jax.shard_map(
        shards,
        mesh=mesh,
        in_specs=(
            P(("freq", "band"), None, None),
            P("freq", None, None, "band"),
            P("freq"),
            P(),
            P(),
            P(("freq", "band")),
        ),
        out_specs=(P("freq", None, None, "band"), P("freq", None, None, None)),
        check_vma=False,
    )
```
